32 devices in a mesh: sp: 16 (over z, y, x), hd: 2 (over core).
Axes of the slice: x: 2, y: 2, z: 4, core: 2. Of those that a mesh axis runs over, the one named last changes fastest.
Arguments:
- frames_in: bfloat16 [16, 32, 8, 512], P(None, 'sp', None, 'hd'), may hold values from -6 to 6
- conv_weight: bfloat16 [3, 3, 3, 512, 512], P(None, None, None, None, 'hd'), may hold values from -0.0546875 to 0.0546875
- conv_out_weight: bfloat16 [3, 3, 3, 512, 16], P(None, None, None, 'hd'), may hold values from -0.0546875 to 0.0546875
- embed_weight: bfloat16 [2, 2, 16, 3072], replicated, may hold values from -0.75 to 0.75
- norm_gain: float32 [3072], replicated, may hold values from 0.25 to 1.75
- q_weight: bfloat16 [3072, 3072], P(None, 'hd'), may hold values from -0.2 to 0.2, as said below
- k_weight: bfloat16 [3072, 3072], P(None, 'hd'), may hold values from -0.2 to 0.2, as said below
- v_weight: bfloat16 [3072, 3072], P(None, 'hd'), may hold values from -0.109375 to 0.109375
- q_gain: float32 [128], replicated, may hold values from 0.5 to 2.5
- k_gain: float32 [128], replicated, may hold values from 0.5 to 2.5
Outputs:
- attention: bfloat16 [1024, 3072], P('sp', 'hd')
- keys: bfloat16 [1024, 3072], P('sp', 'hd')
- values: bfloat16 [1024, 3072], P('sp', 'hd')
The draws below stay inside these ranges and needn't reach their ends.
Inputs may be any that keep to these rules, and one draw needn't show every extreme that they name: `q_weight`: independent entries with a deviation of about one over the square root of 3072. `k_weight`: independent entries with a deviation of about one over the square root of 3072.
All inputs are finite; a program needn't handle non-finite values.
Results may differ from the reference program's by a relative error of at most 0.023.
Values may be sent and summed in bfloat16 or wider, within the bound.
A program may use at most 128 MiB of HBM per device.

```python
import math
import jax
import jax.numpy as jnp
from jax import lax

D = 3072
HEADS = 24
HDIM = 128
CIN = 512
COUT = 512
LATC = 16
FRAMES = 16
HROWS = 32
WCOLS = 8
TOK = 64
TOKENS = 1024


LIMIT = 0.19921875


def projection_pair(key):
    first = jax.random.normal(jax.random.fold_in(key, 11), (D, HEADS * HDIM), jnp.float32)
    second = jax.random.normal(jax.random.fold_in(key, 12), (D, HEADS * HDIM), jnp.float32)
    factor = D ** (-0.5)
    return (jnp.clip(first * factor, -LIMIT, LIMIT), jnp.clip(second * factor, -LIMIT, LIMIT))


def draw_q_weight(key, part):
    return projection_pair(key)[0].astype(jnp.bfloat16)


def draw_k_weight(key, part):
    return projection_pair(key)[1].astype(jnp.bfloat16)


def steps_of(stream_key, extent, shards, low, top_value):
    def one(axis_at, shards_of):
        heights = jax.random.uniform(jax.random.fold_in(jax.random.fold_in(stream_key, 6), axis_at), (shards_of,), jnp.float32, low / len(shards), top_value / len(shards))
        return jnp.repeat(jnp.exp(heights), extent[axis_at] // shards_of).reshape((-1,) + (1,) * (len(extent) - axis_at - 1))

    factor_of = one(*shards[0])
    for cut in shards[1:]:
        factor_of = factor_of * one(*cut)
    return factor_of


def gaussian(rng, extent, scale, most, cuts=(), held_as=jnp.bfloat16):
    array = scale * jax.random.normal(rng, extent, jnp.float32)
    if cuts:
        array = array * steps_of(rng, extent, cuts, -0.22, 0.18)
    return jnp.clip(array, -most, most).astype(held_as)


def setup_inputs(seed: int = 0) -> dict:
    arg_keys = jax.random.split(jax.random.key(seed), 11)
    return {
        "frames_in": gaussian(arg_keys[0], (FRAMES, HROWS, WCOLS, CIN), 1.0, 6.0, ((1, 16), (3, 2))),
        "conv_weight": gaussian(arg_keys[1], (3, 3, 3, CIN, COUT), (27 * CIN) ** -0.5, 0.0546875, ((4, 2),)),
        "conv_out_weight": gaussian(arg_keys[2], (3, 3, 3, COUT, LATC), (27 * COUT) ** -0.5, 0.0546875, ((3, 2),)),
        "embed_weight": gaussian(arg_keys[3], (2, 2, LATC, D), (4 * LATC) ** -0.5, 0.75),
        "norm_gain": jnp.clip(1.0 + 0.15 * jax.random.normal(arg_keys[4], (D,), jnp.float32), 0.25, 1.75),
        "q_weight": draw_q_weight(jax.random.fold_in(arg_keys[10], 71), 0),
        "k_weight": draw_k_weight(jax.random.fold_in(arg_keys[10], 71), 0),
        "v_weight": gaussian(arg_keys[7], (D, HEADS * HDIM), D ** -0.5, 0.109375, ((1, 2),)),
        "q_gain": jnp.clip(jnp.exp(jax.random.uniform(arg_keys[8], (HDIM,), jnp.float32, math.log(0.5), math.log(2.5))), 0.5, 2.5),
        "k_gain": jnp.clip(jnp.exp(jax.random.uniform(arg_keys[9], (HDIM,), jnp.float32, math.log(0.5), math.log(2.5))), 0.5, 2.5),
    }


EPS = 1e-06

def conv_sum(padded, weight, nframe, nrow, ncol):
    width_in = padded.shape[-1]
    total = jnp.zeros((nframe * nrow * ncol, weight.shape[-1]), jnp.float32)
    for step_t in range(3):
        for step_h in range(3):
            for step_w in range(3):
                window = padded[step_t:step_t + nframe, step_h:step_h + nrow, step_w:step_w + ncol]
                total = total + jnp.dot(window.reshape(-1, width_in), weight[step_t, step_h, step_w], preferred_element_type=jnp.float32)
    return total

def patchify(feature):
    nframe, nrow, ncol, width = feature.shape
    shaped = feature.reshape(nframe, nrow // 2, 2, ncol // 2, 2, width)
    shaped = shaped.transpose(0, 1, 3, 2, 4, 5)
    return shaped.reshape(nframe * (nrow // 2) * (ncol // 2), 4 * width)

def rms_scale(value, gain):
    value = value.astype(jnp.float32)
    return value * lax.rsqrt(lax.optimization_barrier(jnp.mean(value * value, axis=-1, keepdims=True)) + EPS) * gain

def reference(frames_in, conv_weight, conv_out_weight, embed_weight, norm_gain, q_weight, k_weight, v_weight, q_gain, k_gain):
    padded = jnp.pad(frames_in, ((2, 0), (1, 1), (1, 1), (0, 0)))
    feature = jax.nn.silu(conv_sum(padded, conv_weight, FRAMES, HROWS, WCOLS)).astype(jnp.bfloat16).reshape(FRAMES, HROWS, WCOLS, COUT)
    padded_feature = jnp.pad(feature, ((2, 0), (1, 1), (1, 1), (0, 0)))
    latent = conv_sum(padded_feature, conv_out_weight, FRAMES, HROWS, WCOLS).astype(jnp.bfloat16).reshape(FRAMES, HROWS, WCOLS, LATC)
    patches = patchify(latent)
    embedded = jnp.dot(patches, embed_weight.reshape(-1, D), preferred_element_type=jnp.float32).astype(jnp.bfloat16)
    normed = rms_scale(embedded, norm_gain).astype(jnp.bfloat16)
    query = jnp.dot(normed, q_weight, preferred_element_type=jnp.float32).reshape(TOKENS, HEADS, HDIM)
    query = rms_scale(query, q_gain).astype(jnp.bfloat16)
    keys = jnp.dot(normed, k_weight, preferred_element_type=jnp.float32).reshape(TOKENS, HEADS, HDIM)
    keys = rms_scale(keys, k_gain).astype(jnp.bfloat16)
    values = jnp.dot(normed, v_weight, preferred_element_type=jnp.float32).astype(jnp.bfloat16)
    values_heads = values.reshape(TOKENS, HEADS, HDIM)
    frame = jnp.arange(TOKENS, dtype=jnp.int32) // TOK
    allowed = frame[:, None] >= frame[None, :]
    scale = HDIM ** (-0.5)

    def one_head(items):
        query_head, key_head, value_head = items
        scores = jnp.dot(query_head, key_head.T, preferred_element_type=jnp.float32) * scale
        scores = jnp.where(allowed, scores, -1e+30)
        top = lax.optimization_barrier(jnp.max(scores, axis=1, keepdims=True))
        weights = jnp.where(allowed, jnp.exp(scores - top), 0.0)
        total = lax.optimization_barrier(jnp.sum(weights, axis=1, keepdims=True))
        mixed = jnp.dot(weights.astype(jnp.bfloat16), value_head, preferred_element_type=jnp.float32)
        return (mixed / total).astype(jnp.bfloat16)
    outputs = lax.map(one_head, (query.transpose(1, 0, 2), keys.transpose(1, 0, 2), values_heads.transpose(1, 0, 2)))
    attention = outputs.transpose(1, 0, 2).reshape(TOKENS, HEADS * HDIM)
    return (attention, keys.reshape(TOKENS, HEADS * HDIM), values)
```

```python
import functools
import math

import jax
import jax.numpy as jnp
from jax import lax
from jax.experimental import pallas as pl
from jax.experimental.pallas import tpu as pltpu
from jax.sharding import PartitionSpec as P

EPS = 1e-06
MESH = pl.DeviceIdType.MESH
ANY_SPEC = pl.BlockSpec(memory_space=pl.ANY)
VMEM_SPEC = pl.BlockSpec(memory_space=pltpu.VMEM)
SPLIT = 4
DEPTH = 3
F32 = jnp.float32
BF16 = jnp.bfloat16


def dot_nt(a, b):
    return lax.dot_general(a, b, (((1,), (1,)), ((), ())), preferred_element_type=F32)


def dot(a, b):
    return jnp.dot(a, b, preferred_element_type=F32)


def encode_kernel(
    count,
    groups,
    x_ref,
    cw_ref,
    w2_ref,
    emb_ref,
    gain_ref,
    wq_ref,
    wk_ref,
    wv_ref,
    gath_out,
    m_out,
    mkt_out,
    gram_out,
    land,
    cwv,
    w2v,
    embv,
    gainv,
    wbuf,
    eb,
    macc,
    mbuf,
    mktbuf,
    grambuf,
    xs,
    acc,
    shift,
    pown,
    pin,
    gbuf,
    in_sem,
    cw_sem,
    w_sem,
    out_sem,
    halo_send,
    halo_recv,
    own_send,
    own_recv,
    fwd_send,
    fwd_recv,
    part_send,
    part_recv,
    gath_send,
    gath_recv,
    relay_send,
    relay_recv,
):
    sp, hd = lax.axis_index("sp"), lax.axis_index("hd")
    nframe, ncol, cl = land.shape[2:]
    pos = nframe * ncol
    depth = eb.shape[1]
    step_rows = depth // SPLIT
    steps = 3 * SPLIT
    lat = w2v.shape[3]
    first, last = sp == 0, sp == count - 1

    rows_in = [
        pltpu.make_async_copy(x_ref.at[:, r], land.at[hd, 1 + r], in_sem.at[r]) for r in range(2)
    ]
    emb_in = pltpu.make_async_copy(emb_ref, embv, in_sem.at[2])
    gain_in = pltpu.make_async_copy(gain_ref, gainv, in_sem.at[3])
    w2_in = pltpu.make_async_copy(w2_ref, w2v, in_sem.at[4])
    cw_in = [
        pltpu.make_async_copy(cw_ref.at[:, dh], cwv.at[:, dh], cw_sem.at[dh]) for dh in range(3)
    ]

    def w_in(i):
        ref = (wq_ref, wk_ref, wv_ref)[i // SPLIT]
        return pltpu.make_async_copy(
            ref.at[pl.ds((i % SPLIT) * step_rows, step_rows)], wbuf.at[i], w_sem.at[i]
        )

    for copy in rows_in + [emb_in, gain_in]:
        copy.start()
    w_in(0).start()
    w_in(1).start()
    w2_in.start()
    for dh in (1, 2, 0):
        cw_in[dh].start()
    w_in(2).start()

    barrier = pltpu.get_barrier_semaphore()
    for k in range(1, count):
        pl.semaphore_signal(
            barrier, inc=1, device_id=(lax.rem(sp + k, count), hd), device_id_type=MESH
        )
    for k in range(1, groups):
        pl.semaphore_signal(
            barrier, inc=1, device_id=(sp, lax.rem(hd + k, groups)), device_id_type=MESH
        )

    def mate(k):
        return (sp, lax.rem(hd + k, groups))

    def remote(src, dst, send, recv, device):
        return pltpu.make_async_remote_copy(
            src_ref=src,
            dst_ref=dst,
            send_sem=send,
            recv_sem=recv,
            device_id=device,
            device_id_type=MESH,
        )

    half = pos // 2
    pcol = ncol // 2
    src = lax.broadcasted_iota(jnp.int32, (pos, pos), 0)
    dst = lax.broadcasted_iota(jnp.int32, (pos, pos), 1)
    odd = dst // half
    frame = (dst % half) // pcol
    column = 2 * (dst % pcol) + odd
    for dt in range(3):
        for dw in range(3):
            c = column + (dw - 1)
            hit = (src == (frame + (dt - 2)) * ncol + c) & (c >= 0) & (c < ncol)
            k = dt * 3 + dw
            shift[k * pos : (k + 1) * pos] = jnp.where(hit, 1.0, 0.0).astype(BF16)
    for g in range(groups):
        for r in range(4):
            xs[g, r, 0 : 2 * ncol] = jnp.zeros((2 * ncol, cl), BF16)

    emb_in.wait()
    gain_in.wait()
    for b in range(2):
        for a in range(2):
            rows = embv[(a * 2 + b) * lat : (a * 2 + b + 1) * lat]
            at = (b * 2 + a) * lat
            eb[at : at + lat] = rows
    gram = dot_nt(eb[...], eb[...]) * (1.0 / depth)
    top = gram.astype(BF16)
    rest = gram - top.astype(F32)
    mid = rest.astype(BF16)
    low = (rest - mid.astype(F32)).astype(BF16)
    wide = eb.shape[0]
    grambuf[0:wide] = top
    grambuf[wide : 2 * wide] = mid
    grambuf[2 * wide : 3 * wide] = low
    eb[...] = (eb[...].astype(F32) * gainv[...]).astype(BF16)

    def m_step(i):
        w_in(i).wait()
        if i + DEPTH < steps:
            w_in(i + DEPTH).start()
        part = i % SPLIT
        value = dot(eb[:, part * step_rows : (part + 1) * step_rows], wbuf[i])
        if part == 0:
            macc[i // SPLIT] = value
        else:
            macc[i // SPLIT] += value

    m_step(0)
    for copy in rows_in:
        copy.wait()
    pl.semaphore_wait(barrier, count - 1 + groups - 1)

    to_prev = remote(
        land.at[hd, 1], land.at[hd, 3], halo_send.at[0], halo_recv.at[0], (lax.rem(sp + count - 1, count), hd)
    )
    to_next = remote(
        land.at[hd, 2], land.at[hd, 0], halo_send.at[1], halo_recv.at[1], (lax.rem(sp + 1, count), hd)
    )

    @pl.when(jnp.logical_not(first))
    def _():
        to_prev.start()

    @pl.when(jnp.logical_not(last))
    def _():
        to_next.start()

    own_out = [
        remote(
            land.at[hd, pl.ds(1, 2)],
            land.at[hd, pl.ds(1, 2)],
            own_send.at[k],
            own_recv.at[k],
            mate(k),
        )
        for k in range(1, groups)
    ]
    for copy in own_out:
        copy.start()

    m_step(1)
    m_step(2)

    def settle(g, r):
        flat = land[g, r].astype(F32).reshape(pos, cl)
        xs[g, r, 2 * ncol :] = flat.astype(BF16)

    for copy in own_out:
        copy.wait_recv()
    for g in range(groups):
        settle(g, 1)
        settle(g, 2)
    for dh in (1, 2, 0):
        cw_in[dh].wait()

    def taps(row, dh, dw):
        total = None
        for g in range(groups):
            for dt in range(3):
                value = dot(
                    xs[g, row, dt * ncol : dt * ncol + pos],
                    cwv[dt, dh, dw, g * cl : (g + 1) * cl],
                )
                total = value if total is None else total + value
        return total

    for dw in range(3):
        acc[dw, 0:pos] = taps(1, 1, dw) + taps(2, 2, dw)
        acc[dw, pos : 2 * pos] = taps(2, 1, dw) + taps(1, 0, dw)

    for i in range(3, 9):
        m_step(i)

    fwd = [
        [
            remote(
                land.at[hd, r],
                land.at[hd, r],
                fwd_send.at[k, r // 3],
                fwd_recv.at[k, r // 3],
                mate(k),
            )
            for k in range(1, groups)
        ]
        for r in (0, 3)
    ]

    @pl.when(jnp.logical_not(first))
    def _():
        to_next.wait_recv()
        for copy in fwd[0]:
            copy.start()

    @pl.when(jnp.logical_not(last))
    def _():
        to_prev.wait_recv()
        for copy in fwd[1]:
            copy.start()

    @pl.when(jnp.logical_not(first))
    def _():
        for copy in fwd[0]:
            copy.wait_recv()
        for g in range(groups):
            settle(g, 0)

    @pl.when(first)
    def _():
        for g in range(groups):
            xs[g, 0, 2 * ncol :] = jnp.zeros((pos, cl), BF16)

    @pl.when(jnp.logical_not(last))
    def _():
        for copy in fwd[1]:
            copy.wait_recv()
        for g in range(groups):
            settle(g, 3)

    @pl.when(last)
    def _():
        for g in range(groups):
            xs[g, 3, 2 * ncol :] = jnp.zeros((pos, cl), BF16)

    summed = []
    for dw in range(3):
        upper = acc[dw, 0:pos] + taps(0, 0, dw)
        lower = acc[dw, pos : 2 * pos] + taps(3, 2, dw)
        summed.append(jnp.concatenate([upper, lower], axis=0))
    width = summed[0].shape[-1]
    cube = (2 * nframe, ncol, width)
    place = lax.broadcasted_iota(jnp.int32, cube, 1)
    left, middle, right = [value.reshape(cube) for value in summed]
    feature = (
        middle
        + jnp.where(place > 0, pltpu.roll(left, 1, 1), 0.0)
        + jnp.where(place < ncol - 1, pltpu.roll(right, ncol - 1, 1), 0.0)
    )
    feature = jax.nn.silu(feature).reshape(2 * pos, width).astype(BF16)
    w2_in.wait()
    z = dot_nt(w2v[...].reshape(27 * lat, width), feature)

    def piece(dt, dh, dw, f):
        at = ((dt * 3 + dh) * 3 + dw) * lat
        return z[at : at + lat, f * pos : (f + 1) * pos]

    spread = []
    for dt in range(3):
        for dw in range(3):
            spread.append(
                jnp.concatenate(
                    [
                        piece(dt, 2, dw, 0),
                        piece(dt, 1, dw, 0) + piece(dt, 2, dw, 1),
                        piece(dt, 0, dw, 0) + piece(dt, 1, dw, 1),
                        piece(dt, 0, dw, 1),
                    ],
                    axis=0,
                )
            )
    spread = jnp.concatenate(spread, axis=1)
    high = spread.astype(BF16)
    low = (spread - high.astype(F32)).astype(BF16)
    moved = dot(high, shift[...]) + dot(low, shift[...])
    pown[...] = moved.reshape(pown.shape)

    parts = [
        remote(
            pown.at[lax.rem(hd + k, groups)],
            pin.at[k],
            part_send.at[k],
            part_recv.at[k],
            mate(k),
        )
        for k in range(1, groups)
    ]
    for copy in parts:
        copy.start()
    total = pown[hd]
    for k in range(1, groups):
        parts[k - 1].wait_recv()
        total = total + pin[k]
    gbuf[sp, hd] = total.astype(BF16)

    gather = [
        remote(
            gbuf.at[sp, hd],
            gbuf.at[sp, hd],
            gath_send.at[k],
            gath_recv.at[k],
            (lax.rem(sp + k, count), hd),
        )
        for k in range(1, count)
    ]
    for copy in gather:
        copy.start()

    for i in range(9, steps):
        m_step(i)
    for w in range(3):
        mbuf[w] = macc[w].astype(BF16)
    mktbuf[...] = macc[1].T.astype(BF16)
    outs = [
        pltpu.make_async_copy(mbuf, m_out, out_sem.at[0]),
        pltpu.make_async_copy(mktbuf, mkt_out, out_sem.at[1]),
        pltpu.make_async_copy(grambuf, gram_out, out_sem.at[2]),
    ]
    for copy in outs:
        copy.start()

    for copy in gather:
        copy.wait_recv()
    relay = [
        remote(gbuf.at[:, hd], gbuf.at[:, hd], relay_send.at[k], relay_recv.at[k], mate(k))
        for k in range(1, groups)
    ]
    for copy in relay:
        copy.start()
    for copy in relay:
        copy.wait_recv()
    result = pltpu.make_async_copy(gbuf, gath_out, out_sem.at[3])
    result.start()

    @pl.when(jnp.logical_not(first))
    def _():
        to_prev.wait_send()
        for copy in fwd[0]:
            copy.wait_send()

    @pl.when(jnp.logical_not(last))
    def _():
        to_next.wait_send()
        for copy in fwd[1]:
            copy.wait_send()

    for copy in own_out + parts + gather + relay:
        copy.wait_send()
    for copy in outs:
        copy.wait()
    result.wait()


def attend_kernel(
    count,
    pcol,
    gath_ref,
    m_ref,
    mkt_ref,
    gram_ref,
    qg_ref,
    kg_ref,
    att_ref,
    key_ref,
    val_ref,
    pt,
):
    sp = lax.axis_index("sp")
    lanes = gath_ref.shape[2]
    half = lanes // 2
    lat = gath_ref.shape[1] // 4
    wide = 4 * lat
    tokens = count * half
    own = count * pcol
    hsize = qg_ref.shape[1]
    heads = m_ref.shape[2] // hsize

    def level(r, a):
        value = gath_ref[r, (1 + a) * lat : (2 + a) * lat].astype(F32)
        if a == 0 and r > 0:
            value = value + gath_ref[r - 1, 3 * lat : 4 * lat].astype(F32)
        if a == 1 and r < count - 1:
            value = value + gath_ref[r + 1, 0:lat].astype(F32)
        return value

    per = max(1, 128 // half)
    for r in range(0, count, per):
        rows = [jnp.concatenate([level(r + j, 0), level(r + j, 1)], axis=0) for j in range(per)]
        if per == 1:
            even, odds = rows[0][:, :half], rows[0][:, half:]
        else:
            lane = lax.broadcasted_iota(jnp.int32, rows[0].shape, 1)
            even = jnp.where(lane < half, rows[0], pltpu.roll(rows[1], half, 1))
            odds = jnp.where(lane < half, pltpu.roll(rows[0], half, 1), rows[1])
        pt[:, r * half : (r + per) * half] = jnp.concatenate([even, odds], axis=0).astype(BF16)

    patches = pt[...]
    row = lax.broadcasted_iota(jnp.int32, (own, tokens), 0)
    lane = lax.broadcasted_iota(jnp.int32, (own, tokens), 1)
    want = (row // pcol) * half + sp * pcol + row % pcol
    pick = jnp.where(lane == want, 1.0, 0.0).astype(BF16)
    mine = dot_nt(pick, patches)
    mine16 = mine.astype(BF16)

    gram = gram_ref[...]
    spread = dot(gram, patches)
    spread = spread[0:wide] + spread[wide : 2 * wide] + spread[2 * wide : 3 * wide]
    square = jnp.sum(spread * patches.astype(F32), axis=0, keepdims=True)
    rs = lax.rsqrt(jnp.maximum(square, 0.0) + EPS)
    own_sq = jnp.zeros((own, 1), F32)
    for part in range(3):
        value = dot_nt(mine16, gram[part * wide : (part + 1) * wide])
        own_sq = own_sq + jnp.sum(value * mine, axis=1, keepdims=True)
    rs_own = lax.rsqrt(jnp.maximum(own_sq, 0.0) + EPS)

    val_ref[...] = (dot(mine16, m_ref[2]) * rs_own).astype(BF16)
    query = dot(mine16, m_ref[0]) * rs_own
    key = dot(mine16, m_ref[1]) * rs_own
    scale = hsize ** (-0.5) * math.log2(math.e)
    frame = (lax.broadcasted_iota(jnp.int32, (1, tokens), 1) % half) // pcol
    bias = jnp.where(frame <= sp, 0.0, -1e30)
    for h in range(heads):
        cols = slice(h * hsize, (h + 1) * hsize)
        q, k = query[:, cols], key[:, cols]
        k = k * lax.rsqrt(jnp.mean(k * k, axis=1, keepdims=True) + EPS) * kg_ref[...]
        key_ref[:, cols] = k.astype(BF16)
        q = q * lax.rsqrt(jnp.mean(q * q, axis=1, keepdims=True) + EPS) * qg_ref[...]
        q = (q * (kg_ref[...] * scale)).astype(BF16)
        narrow = dot_nt(q, m_ref[1, :, cols]).astype(BF16)
        raw = dot(mkt_ref[cols], patches)
        norm = jnp.sum(raw * raw, axis=0, keepdims=True) * (1.0 / hsize)
        factor = rs * lax.rsqrt(rs * rs * norm + EPS)
        scores = dot(narrow, patches) * factor + bias
        peak = jnp.max(scores, axis=1, keepdims=True)
        weights = jnp.exp2(scores - peak)
        total = jnp.sum(weights, axis=1, keepdims=True)
        mixed = dot_nt((weights * rs).astype(BF16), patches)
        high = mixed.astype(BF16)
        low = (mixed - high.astype(F32)).astype(BF16)
        value = dot(high, m_ref[2, :, cols]) + dot(low, m_ref[2, :, cols])
        att_ref[:, cols] = (value / total).astype(BF16)


def on_device(
    frames_in,
    conv_weight,
    conv_out_weight,
    embed_weight,
    norm_gain,
    q_weight,
    k_weight,
    v_weight,
    q_gain,
    k_gain,
):
    count, groups = lax.axis_size("sp"), lax.axis_size("hd")
    nframe, own_rows, ncol, cl = frames_in.shape
    if own_rows != 2 or nframe != count:
        raise ValueError("unsupported shape")
    cin, width = conv_weight.shape[-2:]
    lat = conv_out_weight.shape[-1]
    wide = 4 * lat
    depth, hw = q_weight.shape
    pos = nframe * ncol
    hsize = q_gain.shape[0]
    w2 = conv_out_weight.transpose(0, 1, 2, 4, 3)
    step_rows = depth // SPLIT
    dma = pltpu.SemaphoreType.DMA
    gath, m, mkt, gram = pl.pallas_call(
        functools.partial(encode_kernel, count, groups),
        out_shape=(
            jax.ShapeDtypeStruct((count, groups, wide // groups, pos), BF16),
            jax.ShapeDtypeStruct((3, wide, hw), BF16),
            jax.ShapeDtypeStruct((hw, wide), BF16),
            jax.ShapeDtypeStruct((3 * wide, wide), BF16),
        ),
        in_specs=[ANY_SPEC] * 8,
        out_specs=(ANY_SPEC,) * 4,
        scratch_shapes=[
            pltpu.VMEM((groups, 4, nframe, ncol, cl), BF16),
            pltpu.VMEM((3, 3, 3, cin, width), BF16),
            pltpu.VMEM((3, 3, 3, lat, width), BF16),
            pltpu.VMEM((wide, depth), BF16),
            pltpu.VMEM((1, depth), F32),
            pltpu.VMEM((3 * SPLIT, step_rows, hw), BF16),
            pltpu.VMEM((wide, depth), BF16),
            pltpu.VMEM((3, wide, hw), F32),
            pltpu.VMEM((3, wide, hw), BF16),
            pltpu.VMEM((hw, wide), BF16),
            pltpu.VMEM((3 * wide, wide), BF16),
            pltpu.VMEM((groups, 4, (nframe + 2) * ncol, cl), BF16),
            pltpu.VMEM((3, 2 * pos, width), F32),
            pltpu.VMEM((9 * pos, pos), BF16),
            pltpu.VMEM((groups, wide // groups, pos), F32),
            pltpu.VMEM((groups, wide // groups, pos), F32),
            pltpu.VMEM((count, groups, wide // groups, pos), BF16),
            dma((5,)),
            dma((3,)),
            dma((3 * SPLIT,)),
            dma((4,)),
            dma((2,)),
            dma((2,)),
            dma((groups,)),
            dma((groups,)),
            dma((groups, 2)),
            dma((groups, 2)),
            dma((groups,)),
            dma((groups,)),
            dma((count,)),
            dma((count,)),
            dma((groups,)),
            dma((groups,)),
        ],
        compiler_params=pltpu.CompilerParams(
            collective_id=0, has_side_effects=True, vmem_limit_bytes=56 * 1024 * 1024
        ),
    )(
        frames_in,
        conv_weight,
        w2,
        embed_weight.reshape(wide, depth),
        norm_gain.reshape(1, -1),
        q_weight,
        k_weight,
        v_weight,
    )
    own = count * (ncol // 2)
    shape = jax.ShapeDtypeStruct((own, hw), BF16)
    return pl.pallas_call(
        functools.partial(attend_kernel, count, ncol // 2),
        out_shape=(shape,) * 3,
        in_specs=[VMEM_SPEC] * 6,
        out_specs=(VMEM_SPEC,) * 3,
        scratch_shapes=[pltpu.VMEM((wide, count * pos // 2), BF16)],
        compiler_params=pltpu.CompilerParams(vmem_limit_bytes=48 * 1024 * 1024),
    )(
        gath.reshape(count, wide, pos),
        m,
        mkt,
        gram,
        q_gain.reshape(1, -1),
        k_gain.reshape(1, -1),
    )


def solution(mesh):
    in_specs = (
        P(None, "sp", None, "hd"),
        P(None, None, None, None, "hd"),
        P(None, None, None, "hd", None),
        P(),
        P(),
        P(None, "hd"),
        P(None, "hd"),
        P(None, "hd"),
        P(),
        P(),
    )
    out_specs = (P("sp", "hd"), P("sp", "hd"), P("sp", "hd"))
    return jax.shard_map(
        on_device, mesh=mesh, in_specs=in_specs, out_specs=out_specs, check_vma=False
    )
```

```python
import functools
import math

import jax
import jax.numpy as jnp
from jax import lax
from jax.experimental import pallas as pl
from jax.experimental.pallas import tpu as pltpu
from jax.sharding import PartitionSpec as P

EPS = 1e-06
MESH = pl.DeviceIdType.MESH
ANY_SPEC = pl.BlockSpec(memory_space=pl.ANY)
VMEM_SPEC = pl.BlockSpec(memory_space=pltpu.VMEM)
SPLIT = 4
DEPTH = 5
F32 = jnp.float32
BF16 = jnp.bfloat16


def dot_nt(a, b):
    return lax.dot_general(a, b, (((1,), (1,)), ((), ())), preferred_element_type=F32)


def dot(a, b):
    return jnp.dot(a, b, preferred_element_type=F32)


def encode_kernel(
    count,
    groups,
    x_ref,
    cw_ref,
    w2_ref,
    emb_ref,
    gain_ref,
    wq_ref,
    wk_ref,
    wv_ref,
    gath_out,
    m_out,
    gram_out,
    land,
    cwv,
    w2v,
    embv,
    gainv,
    wbuf,
    eb,
    macc,
    mbuf,
    grambuf,
    xs,
    acc,
    shift,
    pown,
    pin,
    gbuf,
    ready,
    in_sem,
    cw_sem,
    w_sem,
    out_sem,
    halo_send,
    halo_recv,
    own_send,
    own_recv,
    fwd_send,
    fwd_recv,
    part_send,
    part_recv,
    gath_send,
    gath_recv,
    relay_send,
    relay_recv,
):
    sp, hd = lax.axis_index("sp"), lax.axis_index("hd")
    nframe, ncol, cl = land.shape[2:]
    pos = nframe * ncol
    depth = eb.shape[1]
    step_rows = depth // SPLIT
    lat = w2v.shape[3]
    bits = count.bit_length() - 1
    first, last = sp == 0, sp == count - 1

    rows_in = [
        pltpu.make_async_copy(x_ref.at[:, r], land.at[hd, 1 + r], in_sem.at[r]) for r in range(2)
    ]
    emb_in = pltpu.make_async_copy(emb_ref, embv, in_sem.at[2])
    gain_in = pltpu.make_async_copy(gain_ref, gainv, in_sem.at[3])
    w2_in = pltpu.make_async_copy(w2_ref, w2v, in_sem.at[4])
    cw_in = [
        pltpu.make_async_copy(cw_ref.at[:, dh], cwv.at[:, dh], cw_sem.at[dh]) for dh in range(3)
    ]

    def w_in(i):
        w, part = divmod(i, SPLIT)
        at = pl.ds(part * step_rows, step_rows)
        return pltpu.make_async_copy(
            (wq_ref, wk_ref, wv_ref)[w].at[at], wbuf.at[w, at], w_sem.at[i]
        )

    for copy in rows_in + [emb_in, gain_in]:
        copy.start()
    w_in(0).start()
    w_in(1).start()
    for dh in (1, 2, 0):
        cw_in[dh].start()
    w2_in.start()
    for i in range(2, DEPTH):
        w_in(i).start()

    barrier = pltpu.get_barrier_semaphore()
    prev_id, next_id = (jnp.maximum(sp - 1, 0), hd), (jnp.minimum(sp + 1, count - 1), hd)

    def across(k):
        low = sp % (2 * k)
        return (jnp.where(low >= k, sp - k, sp + k), hd)

    def arrive(device):
        pl.semaphore_signal(barrier, inc=1, device_id=device, device_id_type=MESH)

    @pl.when(jnp.logical_not(first))
    def _():
        arrive(prev_id)

    @pl.when(jnp.logical_not(last))
    def _():
        arrive(next_id)

    for bit in range(bits):
        arrive(across(1 << bit))
    for k in range(1, groups):
        arrive((sp, lax.rem(hd + k, groups)))

    def mate(k):
        return (sp, lax.rem(hd + k, groups))

    def remote(src, dst, send, recv, device):
        return pltpu.make_async_remote_copy(
            src_ref=src,
            dst_ref=dst,
            send_sem=send,
            recv_sem=recv,
            device_id=device,
            device_id_type=MESH,
        )

    half = pos // 2
    pcol = ncol // 2
    src = lax.broadcasted_iota(jnp.int32, (pos, pos), 0)
    dst = lax.broadcasted_iota(jnp.int32, (pos, pos), 1)
    odd = dst // half
    frame = (dst % half) // pcol
    column = 2 * (dst % pcol) + odd
    for dt in range(3):
        for dw in range(3):
            c = column + (dw - 1)
            hit = (src == (frame + (dt - 2)) * ncol + c) & (c >= 0) & (c < ncol)
            k = dt * 3 + dw
            shift[k * pos : (k + 1) * pos] = jnp.where(hit, 1.0, 0.0).astype(BF16)
    for g in range(groups):
        for r in range(4):
            xs[g, r, 0 : 2 * ncol] = jnp.zeros((2 * ncol, cl), BF16)

    emb_in.wait()
    gain_in.wait()
    for b in range(2):
        for a in range(2):
            rows = embv[(a * 2 + b) * lat : (a * 2 + b + 1) * lat]
            at = (b * 2 + a) * lat
            eb[at : at + lat] = rows
    wide = eb.shape[0]

    def split3(value):
        lane = lax.broadcasted_iota(jnp.int32, value.shape, 1)
        top = value.astype(BF16).astype(F32)
        rest = value - top
        mid = rest.astype(BF16).astype(F32)
        low = rest - mid
        return jnp.where(lane < wide, top, jnp.where(lane < 2 * wide, mid, low)).astype(BF16)

    def gram_of(rows, size):
        return split3(dot_nt(rows, jnp.concatenate([rows] * 3, axis=0)) * (1.0 / size))

    grambuf[0:wide] = gram_of(eb[...], depth)
    eb[...] = (eb[...].astype(F32) * gainv[...]).astype(BF16)

    def m_step(i):
        w_in(i).wait()
        if i + DEPTH < 3 * SPLIT:
            w_in(i + DEPTH).start()
        w, part = divmod(i, SPLIT)
        at = slice(part * step_rows, (part + 1) * step_rows)
        value = dot(eb[:, at], wbuf[w, at])
        if part == 0:
            macc[w] = value
        else:
            macc[w] += value

    def m_steps(low, high):
        for i in range(low, high):
            m_step(i)

    def tell(bit):
        pl.semaphore_signal(
            ready.at[bit], inc=1, device_id=across(1 << bit), device_id_type=MESH
        )

    def hear(bit):
        pl.semaphore_wait(ready.at[bit], 1)

    for copy in rows_in:
        copy.wait()
    ends = jnp.where(first, 0, 1) + jnp.where(last, 0, 1)
    pl.semaphore_wait(barrier, bits + groups - 1 + ends)

    to_prev = remote(
        land.at[hd, 1], land.at[hd, 3], halo_send.at[0], halo_recv.at[0], prev_id
    )
    to_next = remote(
        land.at[hd, 2], land.at[hd, 0], halo_send.at[1], halo_recv.at[1], next_id
    )

    @pl.when(jnp.logical_not(first))
    def _():
        to_prev.start()

    @pl.when(jnp.logical_not(last))
    def _():
        to_next.start()

    own_out = [
        remote(
            land.at[hd, pl.ds(1, 2)],
            land.at[hd, pl.ds(1, 2)],
            own_send.at[k],
            own_recv.at[k],
            mate(k),
        )
        for k in range(1, groups)
    ]
    for copy in own_out:
        copy.start()

    tell(0)
    m_steps(0, 2)

    def settle(g, r):
        flat = land[g, r].astype(F32).reshape(pos, cl)
        xs[g, r, 2 * ncol :] = flat.astype(BF16)

    for copy in own_out:
        copy.wait_recv()
    for g in range(groups):
        settle(g, 1)
        settle(g, 2)
    for dh in (1, 2, 0):
        cw_in[dh].wait()

    def taps(rows, dh, dw):
        total = None
        for g in range(groups):
            for dt in range(3):
                window = [xs[g, r, dt * ncol : dt * ncol + pos] for r in rows]
                value = dot(
                    window[0] if len(rows) == 1 else jnp.concatenate(window, axis=0),
                    cwv[dt, dh, dw, g * cl : (g + 1) * cl],
                )
                total = value if total is None else total + value
        return total

    def own_taps(dw):
        both = taps((1, 2), 1, dw)
        acc[dw, 0:pos] = both[:pos] + taps((2,), 2, dw)
        acc[dw, pos : 2 * pos] = both[pos:] + taps((1,), 0, dw)

    hear(0)
    tell(1)
    for dw in range(3):
        own_taps(dw)
    step = 2
    for bit in range(1, bits):
        m_steps(step, step + 1)
        step += 1
        hear(bit)
        if bit + 1 < bits:
            tell(bit + 1)
    m_steps(step, 6)

    fwd = [
        [
            remote(
                land.at[hd, r],
                land.at[hd, r],
                fwd_send.at[k, r // 3],
                fwd_recv.at[k, r // 3],
                mate(k),
            )
            for k in range(1, groups)
        ]
        for r in (0, 3)
    ]

    @pl.when(jnp.logical_not(first))
    def _():
        to_next.wait_recv()
        for copy in fwd[0]:
            copy.start()

    @pl.when(jnp.logical_not(last))
    def _():
        to_prev.wait_recv()
        for copy in fwd[1]:
            copy.start()

    m_steps(6, 7)

    @pl.when(jnp.logical_not(first))
    def _():
        for copy in fwd[0]:
            copy.wait_recv()
        for g in range(groups):
            settle(g, 0)

    @pl.when(first)
    def _():
        for g in range(groups):
            xs[g, 0, 2 * ncol :] = jnp.zeros((pos, cl), BF16)

    @pl.when(jnp.logical_not(last))
    def _():
        for copy in fwd[1]:
            copy.wait_recv()
        for g in range(groups):
            settle(g, 3)

    @pl.when(last)
    def _():
        for g in range(groups):
            xs[g, 3, 2 * ncol :] = jnp.zeros((pos, cl), BF16)

    def rim_taps(dw):
        acc[dw, 0:pos] += taps((0,), 0, dw)
        acc[dw, pos : 2 * pos] += taps((3,), 2, dw)

    for dw in range(3):
        rim_taps(dw)
    summed = [acc[dw] for dw in range(3)]
    width = summed[0].shape[-1]
    cube = (2 * nframe, ncol, width)
    place = lax.broadcasted_iota(jnp.int32, cube, 1)
    left, middle, right = [value.reshape(cube) for value in summed]
    feature = (
        middle
        + jnp.where(place > 0, pltpu.roll(left, 1, 1), 0.0)
        + jnp.where(place < ncol - 1, pltpu.roll(right, ncol - 1, 1), 0.0)
    )
    feature = jax.nn.silu(feature).reshape(2 * pos, width).astype(BF16)
    w2_in.wait()
    z = dot_nt(w2v[...].reshape(27 * lat, width), feature)

    def piece(dt, dh, dw, f):
        at = ((dt * 3 + dh) * 3 + dw) * lat
        return z[at : at + lat, f * pos : (f + 1) * pos]

    spread = []
    for dt in range(3):
        for dw in range(3):
            spread.append(
                jnp.concatenate(
                    [
                        piece(dt, 2, dw, 0),
                        piece(dt, 1, dw, 0) + piece(dt, 2, dw, 1),
                        piece(dt, 0, dw, 0) + piece(dt, 1, dw, 1),
                        piece(dt, 0, dw, 1),
                    ],
                    axis=0,
                )
            )
    spread = jnp.concatenate(spread, axis=1)
    high = spread.astype(BF16)
    low = (spread - high.astype(F32)).astype(BF16)
    moved = dot(high, shift[...]) + dot(low, shift[...])
    pown[...] = moved.reshape(pown.shape)

    parts = [
        remote(
            pown.at[lax.rem(hd + k, groups)],
            pin.at[k],
            part_send.at[k],
            part_recv.at[k],
            mate(k),
        )
        for k in range(1, groups)
    ]
    for copy in parts:
        copy.start()
    m_steps(7, 8)
    total = pown[hd]
    for k in range(1, groups):
        parts[k - 1].wait_recv()
        total = total + pin[k]
    gbuf[sp, hd] = total.astype(BF16)

    def flip(k):
        other = sp
        for bit in range(bits):
            if (k >> bit) & 1:
                low = sp % (2 << bit)
                other = other + jnp.where(low >= (1 << bit), -(1 << bit), 1 << bit)
        return other

    gather = [
        remote(
            gbuf.at[sp, hd],
            gbuf.at[sp, hd],
            gath_send.at[k],
            gath_recv.at[k],
            (flip(k), hd),
        )
        for k in range(count - 1, 0, -1)
    ]
    for copy in gather:
        copy.start()

    m_steps(8, 3 * SPLIT)
    for w in range(3):
        mbuf[w] = macc[w].astype(BF16)
    hsize = mbuf.shape[2] // (grambuf.shape[0] // wide - 1)
    for h in range(mbuf.shape[2] // hsize):
        rows = mbuf[1, :, h * hsize : (h + 1) * hsize]
        grambuf[(h + 1) * wide : (h + 2) * wide] = gram_of(rows, hsize)
    outs = [
        pltpu.make_async_copy(mbuf, m_out, out_sem.at[0]),
        pltpu.make_async_copy(grambuf, gram_out, out_sem.at[1]),
    ]
    for copy in outs:
        copy.start()

    for copy in gather:
        copy.wait_recv()
    relay = [
        remote(gbuf.at[:, hd], gath_out.at[:, hd], relay_send.at[k], relay_recv.at[k], mate(k))
        for k in range(1, groups)
    ]
    for copy in relay:
        copy.start()
    result = pltpu.make_async_copy(gbuf.at[:, hd], gath_out.at[:, hd], out_sem.at[2])
    result.start()
    for copy in relay:
        copy.wait_recv()

    @pl.when(jnp.logical_not(first))
    def _():
        to_prev.wait_send()
        for copy in fwd[0]:
            copy.wait_send()

    @pl.when(jnp.logical_not(last))
    def _():
        to_next.wait_send()
        for copy in fwd[1]:
            copy.wait_send()

    for copy in own_out + parts + gather + relay:
        copy.wait_send()
    for copy in outs:
        copy.wait()
    result.wait()


def attend_kernel(
    count,
    pcol,
    gath_hbm,
    m_hbm,
    gram_hbm,
    qg_hbm,
    kg_hbm,
    att_hbm,
    key_hbm,
    val_hbm,
    gath_ref,
    m_ref,
    gram_ref,
    qg_ref,
    kg_ref,
    att_ref,
    key_ref,
    val_ref,
    pt,
    pf,
    pn,
    norm,
    factor,
    left,
    in_sem,
    out_sem,
):
    sp = lax.axis_index("sp")
    loads = [
        pltpu.make_async_copy(src, dst, in_sem.at[i])
        for i, (src, dst) in enumerate(
            (
                (gath_hbm, gath_ref),
                (qg_hbm, qg_ref),
                (kg_hbm, kg_ref),
                (m_hbm, m_ref),
                (gram_hbm, gram_ref),
            )
        )
    ]
    for copy in loads:
        copy.start()
    lanes = gath_ref.shape[2]
    half = lanes // 2
    lat = gath_ref.shape[1] // 4
    wide = 4 * lat
    tokens = count * half
    own = count * pcol
    hsize = qg_ref.shape[1]
    heads = m_ref.shape[2] // hsize
    pair = 2 if heads % 2 == 0 else 1
    deep = pt.shape[0]

    row = lax.broadcasted_iota(jnp.int32, (own, tokens), 0)
    lane = lax.broadcasted_iota(jnp.int32, (own, tokens), 1)
    want = (row // pcol) * half + sp * pcol + row % pcol
    pick = jnp.where(lane == want, 1.0, 0.0).astype(BF16)
    tail = (deep - 3 * wide, tokens)
    frame = (lax.broadcasted_iota(jnp.int32, tail, 1) % half) // pcol
    hidden = (frame > sp) & (lax.broadcasted_iota(jnp.int32, tail, 0) == 0)
    pt[3 * wide : deep] = jnp.where(hidden, -1e30, 0.0).astype(BF16)
    rest = (own, deep - 2 * wide)
    ones = jnp.where(lax.broadcasted_iota(jnp.int32, rest, 1) == wide, 1.0, 0.0).astype(BF16)
    for h in range(heads):
        left[h, :, 2 * wide : deep] = ones

    def level(r, a):
        value = gath_ref[r, (1 + a) * lat : (2 + a) * lat].astype(F32)
        if a == 0 and r > 0:
            value = value + gath_ref[r - 1, 3 * lat : 4 * lat].astype(F32)
        if a == 1 and r < count - 1:
            value = value + gath_ref[r + 1, 0:lat].astype(F32)
        return value

    loads[0].wait()
    per = max(1, 128 // half)
    for r in range(0, count, per):
        rows = [jnp.concatenate([level(r + j, 0), level(r + j, 1)], axis=0) for j in range(per)]
        if per == 1:
            even, odds = rows[0][:, :half], rows[0][:, half:]
        else:
            turn = lax.broadcasted_iota(jnp.int32, rows[0].shape, 1)
            even = jnp.where(turn < half, rows[0], pltpu.roll(rows[1], half, 1))
            odds = jnp.where(turn < half, pltpu.roll(rows[0], half, 1), rows[1])
        block = jnp.concatenate([even, odds], axis=0).astype(BF16)
        at = slice(r * half, (r + per) * half)
        for i in range(3):
            pt[i * wide : (i + 1) * wide, at] = block
        pf[:, at] = block.astype(F32)

    patches = pt[0:wide]
    mine16 = dot_nt(pick, patches).astype(BF16)
    for copy in loads[1:]:
        copy.wait()

    def squares(block):
        spread = dot(gram_ref[block * wide : (block + 1) * wide], pt[0 : 3 * wide])
        return jnp.sum(spread * pf[...], axis=0, keepdims=True)

    rs = lax.rsqrt(jnp.maximum(squares(0), 0.0) + EPS)
    own_rs = jnp.sum(jnp.where(lane == want, rs, 0.0), axis=1, keepdims=True)

    value = dot(mine16, m_ref[2]) * own_rs
    val_ref[...] = value.astype(BF16)
    raw_k = dot(mine16, m_ref[1]) * own_rs
    raw_q = dot(mine16, m_ref[0]) * own_rs
    pn[...] = (pf[...] * rs).astype(BF16)
    scale = hsize ** (-0.5) * math.log2(math.e)

    def unit(value):
        return value * lax.rsqrt(jnp.mean(value * value, axis=1, keepdims=True) + EPS)

    for h in range(heads):
        norm[h : h + 1] = squares(h + 1)
    side = lax.broadcasted_iota(jnp.int32, (own, 2 * wide), 1)
    for h in range(heads):
        cols = slice(h * hsize, (h + 1) * hsize)
        key_ref[:, cols] = (unit(raw_k[:, cols]) * kg_ref[...]).astype(BF16)
        q = (unit(raw_q[:, cols]) * qg_ref[...] * (kg_ref[...] * scale)).astype(BF16)
        mk = m_ref[1, :, cols]
        narrow = dot_nt(q, jnp.concatenate([mk, mk], axis=0))
        top = narrow.astype(BF16).astype(F32)
        left[h, :, 0 : 2 * wide] = jnp.where(side < wide, top, narrow - top).astype(BF16)
    early = [
        pltpu.make_async_copy(key_ref, key_hbm, out_sem.at[0]),
        pltpu.make_async_copy(val_ref, val_hbm, out_sem.at[1]),
    ]
    for copy in early:
        copy.start()
    factor[...] = rs * lax.rsqrt(rs * rs * jnp.maximum(norm[...], 0.0) + EPS)

    def score(step):
        rows = left[step * pair : (step + 1) * pair].reshape(pair * own, deep)
        return dot(rows, pt[...])

    ahead = score(0)
    for step in range(heads // pair):
        scores = ahead
        if step + 1 < heads // pair:
            ahead = score(step + 1)
        soft, totals = [], []
        for j in range(pair):
            h = step * pair + j
            part = scores[j * own : (j + 1) * own] * factor[h : h + 1]
            peak = jnp.max(part, axis=1, keepdims=True)
            weights = jnp.exp2(part - peak)
            totals.append(jnp.sum(weights, axis=1, keepdims=True))
            soft.append(weights.astype(BF16))
        mixed = dot_nt(jnp.concatenate(soft, axis=0), pn[...]).astype(BF16)
        for j in range(pair):
            h = step * pair + j
            cols = slice(h * hsize, (h + 1) * hsize)
            out = dot(mixed[j * own : (j + 1) * own], m_ref[2, :, cols])
            att_ref[:, cols] = (out / totals[j]).astype(BF16)

    late = pltpu.make_async_copy(att_ref, att_hbm, out_sem.at[2])
    late.start()
    for copy in early + [late]:
        copy.wait()


def on_device(
    frames_in,
    conv_weight,
    conv_out_weight,
    embed_weight,
    norm_gain,
    q_weight,
    k_weight,
    v_weight,
    q_gain,
    k_gain,
):
    count, groups = lax.axis_size("sp"), lax.axis_size("hd")
    nframe, own_rows, ncol, cl = frames_in.shape
    if own_rows != 2 or nframe != count or count & (count - 1):
        raise ValueError("unsupported shape")
    cin, width = conv_weight.shape[-2:]
    lat = conv_out_weight.shape[-1]
    wide = 4 * lat
    depth, hw = q_weight.shape
    pos = nframe * ncol
    hsize = q_gain.shape[0]
    w2 = conv_out_weight.transpose(0, 1, 2, 4, 3)
    dma = pltpu.SemaphoreType.DMA
    gath, m, gram = pl.pallas_call(
        functools.partial(encode_kernel, count, groups),
        out_shape=(
            jax.ShapeDtypeStruct((count, groups, wide // groups, pos), BF16),
            jax.ShapeDtypeStruct((3, wide, hw), BF16),
            jax.ShapeDtypeStruct(((hw // hsize + 1) * wide, 3 * wide), BF16),
        ),
        in_specs=[ANY_SPEC] * 8,
        out_specs=(ANY_SPEC,) * 3,
        scratch_shapes=[
            pltpu.VMEM((groups, 4, nframe, ncol, cl), BF16),
            pltpu.VMEM((3, 3, 3, cin, width), BF16),
            pltpu.VMEM((3, 3, 3, lat, width), BF16),
            pltpu.VMEM((wide, depth), BF16),
            pltpu.VMEM((1, depth), F32),
            pltpu.VMEM((3, depth, hw), BF16),
            pltpu.VMEM((wide, depth), BF16),
            pltpu.VMEM((3, wide, hw), F32),
            pltpu.VMEM((3, wide, hw), BF16),
            pltpu.VMEM(((hw // hsize + 1) * wide, 3 * wide), BF16),
            pltpu.VMEM((groups, 4, (nframe + 2) * ncol, cl), BF16),
            pltpu.VMEM((3, 2 * pos, width), F32),
            pltpu.VMEM((9 * pos, pos), BF16),
            pltpu.VMEM((groups, wide // groups, pos), F32),
            pltpu.VMEM((groups, wide // groups, pos), F32),
            pltpu.VMEM((count, groups, wide // groups, pos), BF16),
            pltpu.SemaphoreType.REGULAR((count.bit_length() - 1,)),
            dma((5,)),
            dma((3,)),
            dma((3 * SPLIT,)),
            dma((3,)),
            dma((2,)),
            dma((2,)),
            dma((groups,)),
            dma((groups,)),
            dma((groups, 2)),
            dma((groups, 2)),
            dma((groups,)),
            dma((groups,)),
            dma((count,)),
            dma((count,)),
            dma((groups,)),
            dma((groups,)),
        ],
        compiler_params=pltpu.CompilerParams(
            collective_id=0, has_side_effects=True, vmem_limit_bytes=60 * 1024 * 1024
        ),
    )(
        frames_in,
        conv_weight,
        w2,
        embed_weight.reshape(wide, depth),
        norm_gain.reshape(1, -1),
        q_weight,
        k_weight,
        v_weight,
    )
    own = count * (ncol // 2)
    tokens = count * pos // 2
    heads = hw // hsize
    shape = jax.ShapeDtypeStruct((own, hw), BF16)
    return pl.pallas_call(
        functools.partial(attend_kernel, count, ncol // 2),
        out_shape=(shape,) * 3,
        in_specs=[ANY_SPEC] * 5,
        out_specs=(ANY_SPEC,) * 3,
        scratch_shapes=[
            pltpu.VMEM((count, wide, pos), BF16),
            pltpu.VMEM((3, wide, hw), BF16),
            pltpu.VMEM(((heads + 1) * wide, 3 * wide), BF16),
            pltpu.VMEM((1, hsize), F32),
            pltpu.VMEM((1, hsize), F32),
            pltpu.VMEM((own, hw), BF16),
            pltpu.VMEM((own, hw), BF16),
            pltpu.VMEM((own, hw), BF16),
            pltpu.VMEM((3 * wide + 16, tokens), BF16),
            pltpu.VMEM((wide, tokens), F32),
            pltpu.VMEM((wide, tokens), BF16),
            pltpu.VMEM((heads, tokens), F32),
            pltpu.VMEM((heads, tokens), F32),
            pltpu.VMEM((heads, own, 3 * wide + 16), BF16),
            dma((5,)),
            dma((3,)),
        ],
        compiler_params=pltpu.CompilerParams(vmem_limit_bytes=67043328),
    )(
        gath.reshape(count, wide, pos),
        m,
        gram,
        q_gain.reshape(1, -1),
        k_gain.reshape(1, -1),
    )


def solution(mesh):
    in_specs = (
        P(None, "sp", None, "hd"),
        P(None, None, None, None, "hd"),
        P(None, None, None, "hd", None),
        P(),
        P(),
        P(None, "hd"),
        P(None, "hd"),
        P(None, "hd"),
        P(),
        P(),
    )
    out_specs = (P("sp", "hd"), P("sp", "hd"), P("sp", "hd"))
    return jax.shard_map(
        on_device, mesh=mesh, in_specs=in_specs, out_specs=out_specs, check_vma=False
    )
```

```python
import functools
import math

import jax
import jax.numpy as jnp
from jax import lax
from jax.experimental import pallas as pl
from jax.experimental.pallas import tpu as pltpu
from jax.sharding import PartitionSpec as P

EPS = 1e-06
MESH = pl.DeviceIdType.MESH
ANY_SPEC = pl.BlockSpec(memory_space=pl.ANY)
VMEM_SPEC = pl.BlockSpec(memory_space=pltpu.VMEM)
SPLIT = 2
F32 = jnp.float32
BF16 = jnp.bfloat16


def dot_nt(a, b):
    return lax.dot_general(a, b, (((1,), (1,)), ((), ())), preferred_element_type=F32)


def dot(a, b):
    return jnp.dot(a, b, preferred_element_type=F32)


def encode_kernel(
    count,
    groups,
    share,
    x_ref,
    cw_ref,
    w2_ref,
    emb_ref,
    gain_ref,
    wq_ref,
    wk_ref,
    wv_ref,
    gath_out,
    m_out,
    gram_out,
    land,
    cwv,
    w2v,
    embv,
    gainv,
    wbuf,
    eb,
    macc,
    mbuf,
    grambuf,
    xs,
    acc,
    shift,
    pown,
    pin,
    gbuf,
    ready,
    in_sem,
    cw_sem,
    w_sem,
    out_sem,
    halo_send,
    halo_recv,
    own_send,
    own_recv,
    fwd_send,
    fwd_recv,
    part_send,
    part_recv,
    gath_send,
    gath_recv,
    relay_send,
    relay_recv,
    m_send,
    m_recv,
):
    sp, hd = lax.axis_index("sp"), lax.axis_index("hd")
    nframe, ncol, cl = land.shape[2:]
    pos = nframe * ncol
    depth = eb.shape[1]
    step_rows = depth // SPLIT
    lat = w2v.shape[3]
    bits = count.bit_length() - 1
    first, last = sp == 0, sp == count - 1

    rows_in = [
        pltpu.make_async_copy(x_ref.at[:, r], land.at[hd, 1 + r], in_sem.at[r]) for r in range(2)
    ]
    emb_in = pltpu.make_async_copy(emb_ref, embv, in_sem.at[2])
    gain_in = pltpu.make_async_copy(gain_ref, gainv, in_sem.at[3])
    w2_in = pltpu.make_async_copy(w2_ref, w2v, in_sem.at[4])
    cw_in = [
        pltpu.make_async_copy(cw_ref.at[:, dh], cwv.at[:, dh], cw_sem.at[dh]) for dh in range(3)
    ]

    slot = sp % share
    quarter = wbuf.shape[2]

    def w_in(i):
        w, part = divmod(i, SPLIT)
        at = pl.ds(part * step_rows, step_rows)
        cols = pl.ds(pl.multiple_of(slot * quarter, quarter), quarter)
        ref = (wq_ref, wk_ref, wv_ref)[w]
        return pltpu.make_async_copy(
            ref.at[at] if share == 1 else ref.at[at, cols], wbuf.at[w, at], w_sem.at[i]
        )

    for copy in rows_in + [emb_in, gain_in]:
        copy.start()
    for i in range(3 * SPLIT):
        w_in(i).start()

    barrier = pltpu.get_barrier_semaphore()
    prev_id, next_id = (jnp.maximum(sp - 1, 0), hd), (jnp.minimum(sp + 1, count - 1), hd)

    def across(k):
        low = sp % (2 * k)
        return (jnp.where(low >= k, sp - k, sp + k), hd)

    def arrive(device):
        pl.semaphore_signal(barrier, inc=1, device_id=device, device_id_type=MESH)

    @pl.when(jnp.logical_not(first))
    def _():
        arrive(prev_id)

    @pl.when(jnp.logical_not(last))
    def _():
        arrive(next_id)

    for bit in range(bits):
        arrive(across(1 << bit))
    for k in range(1, groups):
        arrive((sp, lax.rem(hd + k, groups)))

    def mate(k):
        return (sp, lax.rem(hd + k, groups))

    def remote(src, dst, send, recv, device):
        return pltpu.make_async_remote_copy(
            src_ref=src,
            dst_ref=dst,
            send_sem=send,
            recv_sem=recv,
            device_id=device,
            device_id_type=MESH,
        )

    def flip(k):
        other = sp
        for bit in range(bits):
            if (k >> bit) & 1:
                low = sp % (2 << bit)
                other = other + jnp.where(low >= (1 << bit), -(1 << bit), 1 << bit)
        return other

    def tell(bit):
        pl.semaphore_signal(
            ready.at[bit], inc=1, device_id=across(1 << bit), device_id_type=MESH
        )

    def hear(bit):
        pl.semaphore_wait(ready.at[bit], 1)

    for copy in rows_in:
        copy.wait()
    ends = jnp.where(first, 0, 1) + jnp.where(last, 0, 1)
    pl.semaphore_wait(barrier, bits + groups - 1 + ends)

    to_prev = remote(
        land.at[hd, 1], land.at[hd, 3], halo_send.at[0], halo_recv.at[0], prev_id
    )
    to_next = remote(
        land.at[hd, 2], land.at[hd, 0], halo_send.at[1], halo_recv.at[1], next_id
    )

    @pl.when(jnp.logical_not(first))
    def _():
        to_prev.start()

    @pl.when(jnp.logical_not(last))
    def _():
        to_next.start()

    own_out = [
        remote(
            land.at[hd, pl.ds(1, 2)],
            land.at[hd, pl.ds(1, 2)],
            own_send.at[k],
            own_recv.at[k],
            mate(k),
        )
        for k in range(1, groups)
    ]
    for copy in own_out:
        copy.start()

    tell(0)
    half = pos // 2
    pcol = ncol // 2
    src = lax.broadcasted_iota(jnp.int32, (pos, pos), 0)
    dst = lax.broadcasted_iota(jnp.int32, (pos, pos), 1)
    odd = dst // half
    frame = (dst % half) // pcol
    column = 2 * (dst % pcol) + odd
    for dt in range(3):
        for dw in range(3):
            c = column + (dw - 1)
            hit = (src == (frame + (dt - 2)) * ncol + c) & (c >= 0) & (c < ncol)
            k = dt * 3 + dw
            shift[k * pos : (k + 1) * pos] = jnp.where(hit, 1.0, 0.0).astype(BF16)
    for g in range(groups):
        for r in range(4):
            xs[g, r, 0 : 2 * ncol] = jnp.zeros((2 * ncol, cl), BF16)

    emb_in.wait()
    gain_in.wait()
    for b in range(2):
        for a in range(2):
            rows = embv[(a * 2 + b) * lat : (a * 2 + b + 1) * lat]
            at = (b * 2 + a) * lat
            eb[at : at + lat] = rows
    wide = eb.shape[0]

    def split3(value):
        lane = lax.broadcasted_iota(jnp.int32, value.shape, 1)
        top = value.astype(BF16).astype(F32)
        rest = value - top
        mid = rest.astype(BF16).astype(F32)
        low = rest - mid
        return jnp.where(lane < wide, top, jnp.where(lane < 2 * wide, mid, low)).astype(BF16)

    def gram_of(rows, size):
        return split3(dot_nt(rows, jnp.concatenate([rows] * 3, axis=0)) * (1.0 / size))

    grambuf[0:wide] = gram_of(eb[...], depth)
    eb[...] = (eb[...].astype(F32) * gainv[...]).astype(BF16)

    def m_step(i):
        w_in(i).wait()
        if i < 3:
            cw_in[(1, 2, 0)[i]].start()
        if i == 3:
            w2_in.start()
        w, part = divmod(i, SPLIT)
        at = slice(part * step_rows, (part + 1) * step_rows)
        value = dot(eb[:, at], wbuf[w, at])
        if part == 0:
            macc[w] = value
        else:
            mbuf[slot, w] = (macc[w] + value).astype(BF16)

    for i in range(3 * SPLIT):
        m_step(i)
    hear(0)
    tell(1)
    spread_m = [
        remote(mbuf.at[slot], mbuf.at[slot], m_send.at[k], m_recv.at[k], (flip(k), hd))
        for k in range(1, share)
    ]
    for copy in spread_m:
        copy.start()

    def settle(g, r):
        flat = land[g, r].astype(F32).reshape(pos, cl)
        xs[g, r, 2 * ncol :] = flat.astype(BF16)

    for copy in own_out:
        copy.wait_recv()
    for g in range(groups):
        settle(g, 1)
        settle(g, 2)

    def taps(rows, dh, dw):
        total = None
        for g in range(groups):
            for dt in range(3):
                window = [xs[g, r, dt * ncol : dt * ncol + pos] for r in rows]
                value = dot(
                    window[0] if len(rows) == 1 else jnp.concatenate(window, axis=0),
                    cwv[dt, dh, dw, g * cl : (g + 1) * cl],
                )
                total = value if total is None else total + value
        return total

    cw_in[1].wait()
    for dw in range(3):
        acc[dw] = taps((1, 2), 1, dw)
    hear(1)
    if bits > 2:
        tell(2)
    cw_in[2].wait()
    for dw in range(3):
        acc[dw, 0:pos] += taps((2,), 2, dw)
    cw_in[0].wait()
    for dw in range(3):
        acc[dw, pos : 2 * pos] += taps((1,), 0, dw)
    for bit in range(2, bits):
        hear(bit)
        if bit + 1 < bits:
            tell(bit + 1)

    fwd = [
        [
            remote(
                land.at[hd, r],
                land.at[hd, r],
                fwd_send.at[k, r // 3],
                fwd_recv.at[k, r // 3],
                mate(k),
            )
            for k in range(1, groups)
        ]
        for r in (0, 3)
    ]

    @pl.when(jnp.logical_not(first))
    def _():
        to_next.wait_recv()
        for copy in fwd[0]:
            copy.start()

    @pl.when(jnp.logical_not(last))
    def _():
        to_prev.wait_recv()
        for copy in fwd[1]:
            copy.start()

    @pl.when(jnp.logical_not(first))
    def _():
        for copy in fwd[0]:
            copy.wait_recv()
        for g in range(groups):
            settle(g, 0)

    @pl.when(first)
    def _():
        for g in range(groups):
            xs[g, 0, 2 * ncol :] = jnp.zeros((pos, cl), BF16)

    @pl.when(jnp.logical_not(last))
    def _():
        for copy in fwd[1]:
            copy.wait_recv()
        for g in range(groups):
            settle(g, 3)

    @pl.when(last)
    def _():
        for g in range(groups):
            xs[g, 3, 2 * ncol :] = jnp.zeros((pos, cl), BF16)

    def rim_taps(dw):
        acc[dw, 0:pos] += taps((0,), 0, dw)
        acc[dw, pos : 2 * pos] += taps((3,), 2, dw)

    for dw in range(3):
        rim_taps(dw)
    summed = [acc[dw] for dw in range(3)]
    width = summed[0].shape[-1]
    cube = (2 * nframe, ncol, width)
    place = lax.broadcasted_iota(jnp.int32, cube, 1)
    left, middle, right = [value.reshape(cube) for value in summed]
    feature = (
        middle
        + jnp.where(place > 0, pltpu.roll(left, 1, 1), 0.0)
        + jnp.where(place < ncol - 1, pltpu.roll(right, ncol - 1, 1), 0.0)
    )
    feature = jax.nn.silu(feature).reshape(2 * pos, width).astype(BF16)
    w2_in.wait()
    z = dot_nt(w2v[...].reshape(27 * lat, width), feature)

    def piece(dt, dh, dw, f):
        at = ((dt * 3 + dh) * 3 + dw) * lat
        return z[at : at + lat, f * pos : (f + 1) * pos]

    spread = []
    for dt in range(3):
        for dw in range(3):
            spread.append(
                jnp.concatenate(
                    [
                        piece(dt, 2, dw, 0),
                        piece(dt, 1, dw, 0) + piece(dt, 2, dw, 1),
                        piece(dt, 0, dw, 0) + piece(dt, 1, dw, 1),
                        piece(dt, 0, dw, 1),
                    ],
                    axis=0,
                )
            )
    spread = jnp.concatenate(spread, axis=1)
    high = spread.astype(BF16)
    low = (spread - high.astype(F32)).astype(BF16)
    moved = dot(high, shift[...]) + dot(low, shift[...])
    pown[...] = moved.reshape(pown.shape)

    parts = [
        remote(
            pown.at[lax.rem(hd + k, groups)],
            pin.at[k],
            part_send.at[k],
            part_recv.at[k],
            mate(k),
        )
        for k in range(1, groups)
    ]
    for copy in parts:
        copy.start()
    total = pown[hd]
    for k in range(1, groups):
        parts[k - 1].wait_recv()
        total = total + pin[k]
    gbuf[sp, hd] = total.astype(BF16)

    gather = [
        remote(
            gbuf.at[sp, hd],
            gbuf.at[sp, hd],
            gath_send.at[k],
            gath_recv.at[k],
            (flip(k), hd),
        )
        for k in range(count - 1, 0, -1)
    ]
    for copy in gather:
        copy.start()

    for copy in spread_m:
        copy.wait_recv()
    blocks = grambuf.shape[0] // wide - 1
    per = blocks // share
    hsize = quarter // per
    for h in range(blocks):
        cols = slice((h % per) * hsize, (h % per + 1) * hsize)
        rows = mbuf[h // per, 1, :, cols]
        grambuf[(h + 1) * wide : (h + 2) * wide] = gram_of(rows, hsize)
    outs = [
        pltpu.make_async_copy(mbuf, m_out, out_sem.at[0]),
        pltpu.make_async_copy(grambuf, gram_out, out_sem.at[1]),
    ]
    for copy in outs:
        copy.start()

    for copy in gather:
        copy.wait_recv()
    relay = [
        remote(gbuf.at[:, hd], gath_out.at[:, hd], relay_send.at[k], relay_recv.at[k], mate(k))
        for k in range(1, groups)
    ]
    for copy in relay:
        copy.start()
    result = pltpu.make_async_copy(gbuf.at[:, hd], gath_out.at[:, hd], out_sem.at[2])
    result.start()
    for copy in relay:
        copy.wait_recv()

    @pl.when(jnp.logical_not(first))
    def _():
        to_prev.wait_send()
        for copy in fwd[0]:
            copy.wait_send()

    @pl.when(jnp.logical_not(last))
    def _():
        to_next.wait_send()
        for copy in fwd[1]:
            copy.wait_send()

    for copy in own_out + spread_m + parts + gather + relay:
        copy.wait_send()
    for copy in outs:
        copy.wait()
    result.wait()


def attend_kernel(
    count,
    pcol,
    gath_hbm,
    m_hbm,
    gram_hbm,
    qg_hbm,
    kg_hbm,
    att_hbm,
    key_hbm,
    val_hbm,
    gath_ref,
    m_ref,
    gram_ref,
    qg_ref,
    kg_ref,
    att_ref,
    key_ref,
    val_ref,
    pt,
    pf,
    pn,
    norm,
    factor,
    left,
    in_sem,
    out_sem,
):
    sp = lax.axis_index("sp")
    loads = [
        pltpu.make_async_copy(src, dst, in_sem.at[i])
        for i, (src, dst) in enumerate(
            (
                (gath_hbm, gath_ref),
                (qg_hbm, qg_ref),
                (kg_hbm, kg_ref),
                (m_hbm, m_ref),
                (gram_hbm, gram_ref),
            )
        )
    ]
    for copy in loads:
        copy.start()
    lanes = gath_ref.shape[2]
    half = lanes // 2
    lat = gath_ref.shape[1] // 4
    wide = 4 * lat
    tokens = count * half
    own = count * pcol
    hsize = qg_ref.shape[1]
    share = m_ref.shape[0]
    per = m_ref.shape[3] // hsize
    heads = share * per
    pair = 2 if heads % 2 == 0 else 1
    deep = pt.shape[0]

    row = lax.broadcasted_iota(jnp.int32, (own, tokens), 0)
    lane = lax.broadcasted_iota(jnp.int32, (own, tokens), 1)
    want = (row // pcol) * half + sp * pcol + row % pcol
    pick = jnp.where(lane == want, 1.0, 0.0).astype(BF16)
    tail = (deep - 3 * wide, tokens)
    frame = (lax.broadcasted_iota(jnp.int32, tail, 1) % half) // pcol
    hidden = (frame > sp) & (lax.broadcasted_iota(jnp.int32, tail, 0) == 0)
    pt[3 * wide : deep] = jnp.where(hidden, -1e30, 0.0).astype(BF16)
    rest = (own, deep - 2 * wide)
    ones = jnp.where(lax.broadcasted_iota(jnp.int32, rest, 1) == wide, 1.0, 0.0).astype(BF16)
    for h in range(heads):
        left[h, :, 2 * wide : deep] = ones

    def level(r, a):
        value = gath_ref[r, (1 + a) * lat : (2 + a) * lat].astype(F32)
        if a == 0 and r > 0:
            value = value + gath_ref[r - 1, 3 * lat : 4 * lat].astype(F32)
        if a == 1 and r < count - 1:
            value = value + gath_ref[r + 1, 0:lat].astype(F32)
        return value

    loads[0].wait()
    joint = max(1, 128 // half)
    for r in range(0, count, joint):
        rows = [jnp.concatenate([level(r + j, 0), level(r + j, 1)], axis=0) for j in range(joint)]
        if joint == 1:
            even, odds = rows[0][:, :half], rows[0][:, half:]
        else:
            turn = lax.broadcasted_iota(jnp.int32, rows[0].shape, 1)
            even = jnp.where(turn < half, rows[0], pltpu.roll(rows[1], half, 1))
            odds = jnp.where(turn < half, pltpu.roll(rows[0], half, 1), rows[1])
        block = jnp.concatenate([even, odds], axis=0).astype(BF16)
        at = slice(r * half, (r + joint) * half)
        for i in range(3):
            pt[i * wide : (i + 1) * wide, at] = block
        pf[:, at] = block.astype(F32)

    patches = pt[0:wide]
    mine16 = dot_nt(pick, patches).astype(BF16)
    for copy in loads[1:]:
        copy.wait()

    def squares(block):
        spread = dot(gram_ref[block * wide : (block + 1) * wide], pt[0 : 3 * wide])
        return jnp.sum(spread * pf[...], axis=0, keepdims=True)

    rs = lax.rsqrt(jnp.maximum(squares(0), 0.0) + EPS)
    own_rs = jnp.sum(jnp.where(lane == want, rs, 0.0), axis=1, keepdims=True)

    def project(w):
        parts = [dot(mine16, m_ref[i, w]) for i in range(share)]
        return jnp.concatenate(parts, axis=1) * own_rs

    def matrix(w, h):
        return m_ref[h // per, w, :, (h % per) * hsize : (h % per + 1) * hsize]

    val_ref[...] = project(2).astype(BF16)
    raw_k = project(1)
    raw_q = project(0)
    pn[...] = (pf[...] * rs).astype(BF16)
    scale = hsize ** (-0.5) * math.log2(math.e)

    def unit(value):
        return value * lax.rsqrt(jnp.mean(value * value, axis=1, keepdims=True) + EPS)

    for h in range(heads):
        norm[h : h + 1] = squares(h + 1)
    side = lax.broadcasted_iota(jnp.int32, (own, 2 * wide), 1)
    for h in range(heads):
        cols = slice(h * hsize, (h + 1) * hsize)
        key_ref[:, cols] = (unit(raw_k[:, cols]) * kg_ref[...]).astype(BF16)
        q = (unit(raw_q[:, cols]) * qg_ref[...] * (kg_ref[...] * scale)).astype(BF16)
        mk = matrix(1, h)
        narrow = dot_nt(q, jnp.concatenate([mk, mk], axis=0))
        top = narrow.astype(BF16).astype(F32)
        left[h, :, 0 : 2 * wide] = jnp.where(side < wide, top, narrow - top).astype(BF16)
    early = [
        pltpu.make_async_copy(key_ref, key_hbm, out_sem.at[0]),
        pltpu.make_async_copy(val_ref, val_hbm, out_sem.at[1]),
    ]
    for copy in early:
        copy.start()
    factor[...] = rs * lax.rsqrt(rs * rs * jnp.maximum(norm[...], 0.0) + EPS)

    def score(step):
        rows = left[step * pair : (step + 1) * pair].reshape(pair * own, deep)
        return dot(rows, pt[...])

    ahead = score(0)
    for step in range(heads // pair):
        scores = ahead
        if step + 1 < heads // pair:
            ahead = score(step + 1)
        soft, totals = [], []
        for j in range(pair):
            h = step * pair + j
            part = scores[j * own : (j + 1) * own] * factor[h : h + 1]
            peak = jnp.max(part, axis=1, keepdims=True)
            weights = jnp.exp2(part - peak)
            totals.append(jnp.sum(weights, axis=1, keepdims=True))
            soft.append(weights.astype(BF16))
        mixed = dot_nt(jnp.concatenate(soft, axis=0), pn[...]).astype(BF16)
        for j in range(pair):
            h = step * pair + j
            cols = slice(h * hsize, (h + 1) * hsize)
            out = dot(mixed[j * own : (j + 1) * own], matrix(2, h))
            att_ref[:, cols] = (out / totals[j]).astype(BF16)

    late = pltpu.make_async_copy(att_ref, att_hbm, out_sem.at[2])
    late.start()
    for copy in early + [late]:
        copy.wait()


def on_device(
    frames_in,
    conv_weight,
    conv_out_weight,
    embed_weight,
    norm_gain,
    q_weight,
    k_weight,
    v_weight,
    q_gain,
    k_gain,
):
    count, groups = lax.axis_size("sp"), lax.axis_size("hd")
    nframe, own_rows, ncol, cl = frames_in.shape
    if own_rows != 2 or nframe != count or count & (count - 1):
        raise ValueError("unsupported shape")
    cin, width = conv_weight.shape[-2:]
    lat = conv_out_weight.shape[-1]
    wide = 4 * lat
    depth, hw = q_weight.shape
    pos = nframe * ncol
    hsize = q_gain.shape[0]
    w2 = conv_out_weight.transpose(0, 1, 2, 4, 3)
    dma = pltpu.SemaphoreType.DMA
    heads = hw // hsize
    share = 4 if heads % 4 == 0 and count >= 4 else 1
    quarter = hw // share
    gath, m, gram = pl.pallas_call(
        functools.partial(encode_kernel, count, groups, share),
        out_shape=(
            jax.ShapeDtypeStruct((count, groups, wide // groups, pos), BF16),
            jax.ShapeDtypeStruct((share, 3, wide, quarter), BF16),
            jax.ShapeDtypeStruct(((hw // hsize + 1) * wide, 3 * wide), BF16),
        ),
        in_specs=[ANY_SPEC] * 8,
        out_specs=(ANY_SPEC,) * 3,
        scratch_shapes=[
            pltpu.VMEM((groups, 4, nframe, ncol, cl), BF16),
            pltpu.VMEM((3, 3, 3, cin, width), BF16),
            pltpu.VMEM((3, 3, 3, lat, width), BF16),
            pltpu.VMEM((wide, depth), BF16),
            pltpu.VMEM((1, depth), F32),
            pltpu.VMEM((3, depth, quarter), BF16),
            pltpu.VMEM((wide, depth), BF16),
            pltpu.VMEM((3, wide, quarter), F32),
            pltpu.VMEM((share, 3, wide, quarter), BF16),
            pltpu.VMEM(((hw // hsize + 1) * wide, 3 * wide), BF16),
            pltpu.VMEM((groups, 4, (nframe + 2) * ncol, cl), BF16),
            pltpu.VMEM((3, 2 * pos, width), F32),
            pltpu.VMEM((9 * pos, pos), BF16),
            pltpu.VMEM((groups, wide // groups, pos), F32),
            pltpu.VMEM((groups, wide // groups, pos), F32),
            pltpu.VMEM((count, groups, wide // groups, pos), BF16),
            pltpu.SemaphoreType.REGULAR((count.bit_length() - 1,)),
            dma((5,)),
            dma((3,)),
            dma((3 * SPLIT,)),
            dma((3,)),
            dma((2,)),
            dma((2,)),
            dma((groups,)),
            dma((groups,)),
            dma((groups, 2)),
            dma((groups, 2)),
            dma((groups,)),
            dma((groups,)),
            dma((count,)),
            dma((count,)),
            dma((groups,)),
            dma((groups,)),
            dma((share,)),
            dma((share,)),
        ],
        compiler_params=pltpu.CompilerParams(
            collective_id=0, has_side_effects=True, vmem_limit_bytes=60 * 1024 * 1024
        ),
    )(
        frames_in,
        conv_weight,
        w2,
        embed_weight.reshape(wide, depth),
        norm_gain.reshape(1, -1),
        q_weight,
        k_weight,
        v_weight,
    )
    own = count * (ncol // 2)
    tokens = count * pos // 2
    shape = jax.ShapeDtypeStruct((own, hw), BF16)
    return pl.pallas_call(
        functools.partial(attend_kernel, count, ncol // 2),
        out_shape=(shape,) * 3,
        in_specs=[ANY_SPEC] * 5,
        out_specs=(ANY_SPEC,) * 3,
        scratch_shapes=[
            pltpu.VMEM((count, wide, pos), BF16),
            pltpu.VMEM((share, 3, wide, quarter), BF16),
            pltpu.VMEM(((heads + 1) * wide, 3 * wide), BF16),
            pltpu.VMEM((1, hsize), F32),
            pltpu.VMEM((1, hsize), F32),
            pltpu.VMEM((own, hw), BF16),
            pltpu.VMEM((own, hw), BF16),
            pltpu.VMEM((own, hw), BF16),
            pltpu.VMEM((3 * wide + 16, tokens), BF16),
            pltpu.VMEM((wide, tokens), F32),
            pltpu.VMEM((wide, tokens), BF16),
            pltpu.VMEM((heads, tokens), F32),
            pltpu.VMEM((heads, tokens), F32),
            pltpu.VMEM((heads, own, 3 * wide + 16), BF16),
            dma((5,)),
            dma((3,)),
        ],
        compiler_params=pltpu.CompilerParams(vmem_limit_bytes=67043328),
    )(
        gath.reshape(count, wide, pos),
        m,
        gram,
        q_gain.reshape(1, -1),
        k_gain.reshape(1, -1),
    )


def solution(mesh):
    in_specs = (
        P(None, "sp", None, "hd"),
        P(None, None, None, None, "hd"),
        P(None, None, None, "hd", None),
        P(),
        P(),
        P(None, "hd"),
        P(None, "hd"),
        P(None, "hd"),
        P(),
        P(),
    )
    out_specs = (P("sp", "hd"), P("sp", "hd"), P("sp", "hd"))
    return jax.shard_map(
        on_device, mesh=mesh, in_specs=in_specs, out_specs=out_specs, check_vma=False
    )
```

```python
import functools
import math

import jax
import jax.numpy as jnp
from jax import lax
from jax.experimental import pallas as pl
from jax.experimental.pallas import tpu as pltpu
from jax.sharding import PartitionSpec as P

EPS = 1e-06
MESH = pl.DeviceIdType.MESH
ANY_SPEC = pl.BlockSpec(memory_space=pl.ANY)
VMEM_SPEC = pl.BlockSpec(memory_space=pltpu.VMEM)
SPLIT = 2
F32 = jnp.float32
BF16 = jnp.bfloat16


def dot_nt(a, b):
    return lax.dot_general(a, b, (((1,), (1,)), ((), ())), preferred_element_type=F32)


def dot(a, b):
    return jnp.dot(a, b, preferred_element_type=F32)


def encode_kernel(
    count,
    groups,
    share,
    x_ref,
    cw_ref,
    w2_ref,
    emb_ref,
    gain_ref,
    wq_ref,
    wk_ref,
    wv_ref,
    gath_out,
    m_out,
    gram_out,
    land,
    cwv,
    w2v,
    embv,
    gainv,
    wbuf,
    eb,
    macc,
    mbuf,
    grambuf,
    xs,
    acc,
    shift,
    pown,
    pin,
    gbuf,
    ready,
    in_sem,
    cw_sem,
    w_sem,
    out_sem,
    halo_send,
    halo_recv,
    own_send,
    own_recv,
    fwd_send,
    fwd_recv,
    part_send,
    part_recv,
    gath_send,
    gath_recv,
    relay_send,
    relay_recv,
    m_send,
    m_recv,
):
    sp, hd = lax.axis_index("sp"), lax.axis_index("hd")
    nframe, ncol, cl = land.shape[2:]
    pos = nframe * ncol
    depth = eb.shape[1]
    step_rows = depth // SPLIT
    lat = w2v.shape[3]
    bits = count.bit_length() - 1
    first, last = sp == 0, sp == count - 1

    rows_in = [
        pltpu.make_async_copy(x_ref.at[:, r], land.at[hd, 1 + r], in_sem.at[r]) for r in range(2)
    ]
    emb_in = pltpu.make_async_copy(emb_ref, embv, in_sem.at[2])
    gain_in = pltpu.make_async_copy(gain_ref, gainv, in_sem.at[3])
    w2_in = pltpu.make_async_copy(w2_ref, w2v, in_sem.at[4])
    cw_in = [
        pltpu.make_async_copy(cw_ref.at[:, dh], cwv.at[:, dh], cw_sem.at[dh]) for dh in range(3)
    ]

    slot = sp % share
    quarter = wbuf.shape[2]

    def w_in(i):
        w, part = divmod(i, SPLIT)
        at = pl.ds(part * step_rows, step_rows)
        cols = pl.ds(pl.multiple_of(slot * quarter, quarter), quarter)
        ref = (wq_ref, wk_ref, wv_ref)[w]
        return pltpu.make_async_copy(
            ref.at[at] if share == 1 else ref.at[at, cols], wbuf.at[w, at], w_sem.at[i]
        )

    for copy in rows_in + [emb_in, gain_in]:
        copy.start()
    for i in range(3 * SPLIT):
        w_in(i).start()
    barrier = pltpu.get_barrier_semaphore()
    prev_id, next_id = (jnp.maximum(sp - 1, 0), hd), (jnp.minimum(sp + 1, count - 1), hd)

    def across(k):
        low = sp % (2 * k)
        return (jnp.where(low >= k, sp - k, sp + k), hd)

    def arrive(device):
        pl.semaphore_signal(barrier, inc=1, device_id=device, device_id_type=MESH)

    @pl.when(jnp.logical_not(first))
    def _():
        arrive(prev_id)

    @pl.when(jnp.logical_not(last))
    def _():
        arrive(next_id)

    for bit in range(bits):
        arrive(across(1 << bit))
    for k in range(1, groups):
        arrive((sp, lax.rem(hd + k, groups)))

    def mate(k):
        return (sp, lax.rem(hd + k, groups))

    def remote(src, dst, send, recv, device):
        return pltpu.make_async_remote_copy(
            src_ref=src,
            dst_ref=dst,
            send_sem=send,
            recv_sem=recv,
            device_id=device,
            device_id_type=MESH,
        )

    def flip(k):
        other = sp
        for bit in range(bits):
            if (k >> bit) & 1:
                low = sp % (2 << bit)
                other = other + jnp.where(low >= (1 << bit), -(1 << bit), 1 << bit)
        return other

    def tell(bit):
        pl.semaphore_signal(
            ready.at[bit], inc=1, device_id=across(1 << bit), device_id_type=MESH
        )

    def hear(bit):
        pl.semaphore_wait(ready.at[bit], 1)

    for copy in rows_in:
        copy.wait()
    ends = jnp.where(first, 0, 1) + jnp.where(last, 0, 1)
    pl.semaphore_wait(barrier, bits + groups - 1 + ends)

    to_prev = remote(
        land.at[hd, 1], land.at[hd, 3], halo_send.at[0], halo_recv.at[0], prev_id
    )
    to_next = remote(
        land.at[hd, 2], land.at[hd, 0], halo_send.at[1], halo_recv.at[1], next_id
    )

    @pl.when(jnp.logical_not(first))
    def _():
        to_prev.start()

    @pl.when(jnp.logical_not(last))
    def _():
        to_next.start()

    own_out = [
        remote(
            land.at[hd, pl.ds(1, 2)],
            land.at[hd, pl.ds(1, 2)],
            own_send.at[k],
            own_recv.at[k],
            mate(k),
        )
        for k in range(1, groups)
    ]
    for copy in own_out:
        copy.start()

    tell(0)
    half = pos // 2
    pcol = ncol // 2
    src = lax.broadcasted_iota(jnp.int32, (pos, pos), 0)
    dst = lax.broadcasted_iota(jnp.int32, (pos, pos), 1)
    odd = dst // half
    frame = (dst % half) // pcol
    column = 2 * (dst % pcol) + odd
    for dt in range(3):
        for dw in range(3):
            c = column + (dw - 1)
            hit = (src == (frame + (dt - 2)) * ncol + c) & (c >= 0) & (c < ncol)
            k = dt * 3 + dw
            shift[k * pos : (k + 1) * pos] = jnp.where(hit, 1.0, 0.0).astype(BF16)
    for g in range(groups):
        for r in range(4):
            xs[g, r, 0 : 2 * ncol] = jnp.zeros((2 * ncol, cl), BF16)

    emb_in.wait()
    gain_in.wait()
    for b in range(2):
        for a in range(2):
            rows = embv[(a * 2 + b) * lat : (a * 2 + b + 1) * lat]
            at = (b * 2 + a) * lat
            eb[at : at + lat] = rows
    wide = eb.shape[0]

    def split3(value):
        lane = lax.broadcasted_iota(jnp.int32, value.shape, 1)
        top = value.astype(BF16).astype(F32)
        rest = value - top
        mid = rest.astype(BF16).astype(F32)
        low = rest - mid
        return jnp.where(lane < wide, top, jnp.where(lane < 2 * wide, mid, low)).astype(BF16)

    def gram_of(rows, size):
        return split3(dot_nt(rows, jnp.concatenate([rows] * 3, axis=0)) * (1.0 / size))

    grambuf[0:wide] = gram_of(eb[...], depth)
    eb[...] = (eb[...].astype(F32) * gainv[...]).astype(BF16)

    def m_step(i):
        w_in(i).wait()
        if i < 3:
            cw_in[(1, 2, 0)[i]].start()
        if i == 3:
            w2_in.start()
        w, part = divmod(i, SPLIT)
        at = slice(part * step_rows, (part + 1) * step_rows)
        value = dot(eb[:, at], wbuf[w, at])
        if part == 0:
            macc[w] = value
        else:
            mbuf[slot, w] = (macc[w] + value).astype(BF16)

    for i in range(3 * SPLIT):
        m_step(i)
    hear(0)
    tell(1)
    spread_m = [
        remote(mbuf.at[slot], mbuf.at[slot], m_send.at[k], m_recv.at[k], (flip(k), hd))
        for k in range(1, share)
    ]
    for copy in spread_m:
        copy.start()

    def settle(g, r):
        flat = land[g, r].astype(F32).reshape(pos, cl)
        xs[g, r, 2 * ncol :] = flat.astype(BF16)

    for copy in own_out:
        copy.wait_recv()
    for g in range(groups):
        settle(g, 1)
        settle(g, 2)

    def taps(rows, dh, dw, which=range(groups)):
        total = None
        for g in which:
            at = g * cl if isinstance(g, int) else pl.multiple_of(g * cl, cl)
            for dt in range(3):
                window = [xs[g, r, dt * ncol : dt * ncol + pos] for r in rows]
                value = dot(
                    window[0] if len(rows) == 1 else jnp.concatenate(window, axis=0),
                    cwv[dt, dh, dw, pl.ds(at, cl)],
                )
                total = value if total is None else total + value
        return total

    cw_in[1].wait()
    for dw in range(3):
        acc[dw] = taps((1, 2), 1, dw)
    hear(1)
    if bits > 2:
        tell(2)
    cw_in[2].wait()
    for dw in range(3):
        acc[dw, 0:pos] += taps((2,), 2, dw)
    cw_in[0].wait()
    for dw in range(3):
        acc[dw, pos : 2 * pos] += taps((1,), 0, dw)
    for bit in range(2, bits):
        hear(bit)
        if bit + 1 < bits:
            tell(bit + 1)

    fwd = [
        [
            remote(
                land.at[hd, r],
                land.at[hd, r],
                fwd_send.at[k, r // 3],
                fwd_recv.at[k, r // 3],
                mate(k),
            )
            for k in range(1, groups)
        ]
        for r in (0, 3)
    ]

    @pl.when(jnp.logical_not(first))
    def _():
        to_next.wait_recv()
        for copy in fwd[0]:
            copy.start()
        settle(hd, 0)

    @pl.when(jnp.logical_not(last))
    def _():
        to_prev.wait_recv()
        for copy in fwd[1]:
            copy.start()
        settle(hd, 3)

    @pl.when(first)
    def _():
        for g in range(groups):
            xs[g, 0, 2 * ncol :] = jnp.zeros((pos, cl), BF16)

    @pl.when(last)
    def _():
        for g in range(groups):
            xs[g, 3, 2 * ncol :] = jnp.zeros((pos, cl), BF16)

    def rim_taps(which):
        for dw in range(3):
            acc[dw, 0:pos] += taps((0,), 0, dw, which)
            acc[dw, pos : 2 * pos] += taps((3,), 2, dw, which)

    others = [lax.rem(hd + k, groups) for k in range(1, groups)]
    rim_taps([hd])

    @pl.when(jnp.logical_not(first))
    def _():
        for copy in fwd[0]:
            copy.wait_recv()
        for g in others:
            settle(g, 0)

    @pl.when(jnp.logical_not(last))
    def _():
        for copy in fwd[1]:
            copy.wait_recv()
        for g in others:
            settle(g, 3)

    rim_taps(others)
    summed = [acc[dw] for dw in range(3)]
    width = summed[0].shape[-1]
    cube = (2 * nframe, ncol, width)
    place = lax.broadcasted_iota(jnp.int32, cube, 1)
    left, middle, right = [value.reshape(cube) for value in summed]
    feature = (
        middle
        + jnp.where(place > 0, pltpu.roll(left, 1, 1), 0.0)
        + jnp.where(place < ncol - 1, pltpu.roll(right, ncol - 1, 1), 0.0)
    )
    feature = jax.nn.silu(feature).reshape(2 * pos, width).astype(BF16)
    w2_in.wait()
    z = dot_nt(w2v[...].reshape(27 * lat, width), feature)

    def piece(dt, dh, dw, f):
        at = ((dt * 3 + dh) * 3 + dw) * lat
        return z[at : at + lat, f * pos : (f + 1) * pos]

    spread = []
    for dt in range(3):
        for dw in range(3):
            spread.append(
                jnp.concatenate(
                    [
                        piece(dt, 2, dw, 0),
                        piece(dt, 1, dw, 0) + piece(dt, 2, dw, 1),
                        piece(dt, 0, dw, 0) + piece(dt, 1, dw, 1),
                        piece(dt, 0, dw, 1),
                    ],
                    axis=0,
                )
            )
    spread = jnp.concatenate(spread, axis=1)
    high = spread.astype(BF16)
    low = (spread - high.astype(F32)).astype(BF16)
    moved = dot(high, shift[...]) + dot(low, shift[...])
    pown[...] = moved.reshape(pown.shape)

    parts = [
        remote(
            pown.at[lax.rem(hd + k, groups)],
            pin.at[k],
            part_send.at[k],
            part_recv.at[k],
            mate(k),
        )
        for k in range(1, groups)
    ]
    for copy in parts:
        copy.start()
    total = pown[hd]
    for k in range(1, groups):
        parts[k - 1].wait_recv()
        total = total + pin[k]
    gbuf[sp, hd] = total.astype(BF16)

    gather = [
        remote(
            gbuf.at[sp, hd],
            gbuf.at[sp, hd],
            gath_send.at[k],
            gath_recv.at[k],
            (flip(k), hd),
        )
        for k in range(count - 1, 0, -1)
    ]
    for copy in gather:
        copy.start()

    for copy in spread_m:
        copy.wait_recv()
    blocks = grambuf.shape[0] // wide - 1
    per = blocks // share
    hsize = quarter // per
    for h in range(blocks):
        cols = slice((h % per) * hsize, (h % per + 1) * hsize)
        rows = mbuf[h // per, 1, :, cols]
        grambuf[(h + 1) * wide : (h + 2) * wide] = gram_of(rows, hsize)
    outs = [
        pltpu.make_async_copy(mbuf, m_out, out_sem.at[0]),
        pltpu.make_async_copy(grambuf, gram_out, out_sem.at[1]),
    ]
    for copy in outs:
        copy.start()

    for copy in gather:
        copy.wait_recv()
    relay = [
        remote(gbuf.at[:, hd], gath_out.at[:, hd], relay_send.at[k], relay_recv.at[k], mate(k))
        for k in range(1, groups)
    ]
    for copy in relay:
        copy.start()
    result = pltpu.make_async_copy(gbuf.at[:, hd], gath_out.at[:, hd], out_sem.at[2])
    result.start()
    for copy in relay:
        copy.wait_recv()

    @pl.when(jnp.logical_not(first))
    def _():
        to_prev.wait_send()
        for copy in fwd[0]:
            copy.wait_send()

    @pl.when(jnp.logical_not(last))
    def _():
        to_next.wait_send()
        for copy in fwd[1]:
            copy.wait_send()

    for copy in own_out + spread_m + parts + gather + relay:
        copy.wait_send()
    for copy in outs:
        copy.wait()
    result.wait()


def attend_kernel(
    count,
    pcol,
    gath_hbm,
    m_hbm,
    gram_hbm,
    qg_hbm,
    kg_hbm,
    att_hbm,
    key_hbm,
    val_hbm,
    gath_ref,
    m_ref,
    gram_ref,
    qg_ref,
    kg_ref,
    att_ref,
    key_ref,
    val_ref,
    pt,
    pf,
    pn,
    norm,
    factor,
    left,
    in_sem,
    out_sem,
):
    sp = lax.axis_index("sp")
    loads = [
        pltpu.make_async_copy(src, dst, in_sem.at[i])
        for i, (src, dst) in enumerate(
            (
                (gath_hbm, gath_ref),
                (qg_hbm, qg_ref),
                (kg_hbm, kg_ref),
                (m_hbm, m_ref),
                (gram_hbm, gram_ref),
            )
        )
    ]
    for copy in loads:
        copy.start()
    lanes = gath_ref.shape[2]
    half = lanes // 2
    lat = gath_ref.shape[1] // 4
    wide = 4 * lat
    tokens = count * half
    own = count * pcol
    hsize = qg_ref.shape[1]
    share = m_ref.shape[0]
    per = m_ref.shape[3] // hsize
    heads = share * per
    pair = 4 if heads % 4 == 0 else 1
    deep = pt.shape[0]

    row = lax.broadcasted_iota(jnp.int32, (own, tokens), 0)
    lane = lax.broadcasted_iota(jnp.int32, (own, tokens), 1)
    want = (row // pcol) * half + sp * pcol + row % pcol
    pick = jnp.where(lane == want, 1.0, 0.0).astype(BF16)
    tail = (deep - 3 * wide, tokens)
    frame = (lax.broadcasted_iota(jnp.int32, tail, 1) % half) // pcol
    hidden = (frame > sp) & (lax.broadcasted_iota(jnp.int32, tail, 0) == 0)
    pt[3 * wide : deep] = jnp.where(hidden, -1e30, 0.0).astype(BF16)
    rest = (own, deep - 2 * wide)
    ones = jnp.where(lax.broadcasted_iota(jnp.int32, rest, 1) == wide, 1.0, 0.0).astype(BF16)
    for h in range(heads):
        left[h, :, 2 * wide : deep] = ones

    def level(r, a):
        value = gath_ref[r, (1 + a) * lat : (2 + a) * lat].astype(F32)
        if a == 0 and r > 0:
            value = value + gath_ref[r - 1, 3 * lat : 4 * lat].astype(F32)
        if a == 1 and r < count - 1:
            value = value + gath_ref[r + 1, 0:lat].astype(F32)
        return value

    loads[0].wait()
    joint = max(1, 128 // half)
    for r in range(0, count, joint):
        rows = [jnp.concatenate([level(r + j, 0), level(r + j, 1)], axis=0) for j in range(joint)]
        if joint == 1:
            even, odds = rows[0][:, :half], rows[0][:, half:]
        else:
            turn = lax.broadcasted_iota(jnp.int32, rows[0].shape, 1)
            even = jnp.where(turn < half, rows[0], pltpu.roll(rows[1], half, 1))
            odds = jnp.where(turn < half, pltpu.roll(rows[0], half, 1), rows[1])
        block = jnp.concatenate([even, odds], axis=0).astype(BF16)
        at = slice(r * half, (r + joint) * half)
        for i in range(3):
            pt[i * wide : (i + 1) * wide, at] = block
        pf[:, at] = block.astype(F32)

    patches = pt[0:wide]
    mine16 = dot_nt(pick, patches).astype(BF16)
    for copy in loads[1:]:
        copy.wait()

    span = min(tokens, 256)
    for at in range(0, tokens, span):
        cols = slice(at, at + span)
        spread = dot(gram_ref[...], pt[0 : 3 * wide, cols]).reshape(heads + 1, wide, span)
        norm[:, cols] = jnp.maximum(jnp.sum(spread * pf[:, cols][None], axis=1), 0.0)
    rs = lax.rsqrt(norm[0:1] + EPS)
    own_rs = jnp.sum(jnp.where(lane == want, rs, 0.0), axis=1, keepdims=True)

    def project(w):
        parts = [dot(mine16, m_ref[i, w]) for i in range(share)]
        return jnp.concatenate(parts, axis=1) * own_rs

    def matrix(w, h):
        return m_ref[h // per, w, :, (h % per) * hsize : (h % per + 1) * hsize]

    val_ref[...] = project(2).astype(BF16)
    raw_k = project(1)
    raw_q = project(0)
    pn[...] = (pf[...] * rs).astype(BF16)
    scale = hsize ** (-0.5) * math.log2(math.e)

    def unit(value):
        return value * lax.rsqrt(jnp.mean(value * value, axis=1, keepdims=True) + EPS)

    side = lax.broadcasted_iota(jnp.int32, (own, 2 * wide), 1)
    for h in range(heads):
        cols = slice(h * hsize, (h + 1) * hsize)
        key_ref[:, cols] = (unit(raw_k[:, cols]) * kg_ref[...]).astype(BF16)
        q = (unit(raw_q[:, cols]) * qg_ref[...] * (kg_ref[...] * scale)).astype(BF16)
        mk = matrix(1, h)
        narrow = dot_nt(q, jnp.concatenate([mk, mk], axis=0))
        top = narrow.astype(BF16).astype(F32)
        left[h, :, 0 : 2 * wide] = jnp.where(side < wide, top, narrow - top).astype(BF16)
    early = [
        pltpu.make_async_copy(key_ref, key_hbm, out_sem.at[0]),
        pltpu.make_async_copy(val_ref, val_hbm, out_sem.at[1]),
    ]
    for copy in early:
        copy.start()
    factor[...] = rs * lax.rsqrt(rs * rs * norm[1 : heads + 1] + EPS)

    def score(step):
        rows = left[step * pair : (step + 1) * pair].reshape(pair * own, deep)
        return dot(rows, pt[...])

    ahead = score(0)
    for step in range(heads // pair):
        scores = ahead
        if step + 1 < heads // pair:
            ahead = score(step + 1)
        soft, totals = [], []
        for j in range(pair):
            h = step * pair + j
            part = scores[j * own : (j + 1) * own] * factor[h : h + 1]
            peak = jnp.max(part, axis=1, keepdims=True)
            weights = jnp.exp2(part - peak)
            totals.append(jnp.sum(weights, axis=1, keepdims=True))
            soft.append(weights.astype(BF16))
        mixed = dot_nt(jnp.concatenate(soft, axis=0), pn[...]).astype(BF16)
        for j in range(pair):
            h = step * pair + j
            cols = slice(h * hsize, (h + 1) * hsize)
            out = dot(mixed[j * own : (j + 1) * own], matrix(2, h))
            att_ref[:, cols] = (out / totals[j]).astype(BF16)

    late = pltpu.make_async_copy(att_ref, att_hbm, out_sem.at[2])
    late.start()
    for copy in early + [late]:
        copy.wait()


def on_device(
    frames_in,
    conv_weight,
    conv_out_weight,
    embed_weight,
    norm_gain,
    q_weight,
    k_weight,
    v_weight,
    q_gain,
    k_gain,
):
    count, groups = lax.axis_size("sp"), lax.axis_size("hd")
    nframe, own_rows, ncol, cl = frames_in.shape
    if own_rows != 2 or nframe != count or count & (count - 1):
        raise ValueError("unsupported shape")
    cin, width = conv_weight.shape[-2:]
    lat = conv_out_weight.shape[-1]
    wide = 4 * lat
    depth, hw = q_weight.shape
    pos = nframe * ncol
    hsize = q_gain.shape[0]
    w2 = conv_out_weight.transpose(0, 1, 2, 4, 3)
    dma = pltpu.SemaphoreType.DMA
    heads = hw // hsize
    share = 4 if heads % 4 == 0 and count >= 4 else 1
    quarter = hw // share
    gath, m, gram = pl.pallas_call(
        functools.partial(encode_kernel, count, groups, share),
        out_shape=(
            jax.ShapeDtypeStruct((count, groups, wide // groups, pos), BF16),
            jax.ShapeDtypeStruct((share, 3, wide, quarter), BF16),
            jax.ShapeDtypeStruct(((hw // hsize + 1) * wide, 3 * wide), BF16),
        ),
        in_specs=[ANY_SPEC] * 8,
        out_specs=(ANY_SPEC,) * 3,
        scratch_shapes=[
            pltpu.VMEM((groups, 4, nframe, ncol, cl), BF16),
            pltpu.VMEM((3, 3, 3, cin, width), BF16),
            pltpu.VMEM((3, 3, 3, lat, width), BF16),
            pltpu.VMEM((wide, depth), BF16),
            pltpu.VMEM((1, depth), F32),
            pltpu.VMEM((3, depth, quarter), BF16),
            pltpu.VMEM((wide, depth), BF16),
            pltpu.VMEM((3, wide, quarter), F32),
            pltpu.VMEM((share, 3, wide, quarter), BF16),
            pltpu.VMEM(((hw // hsize + 1) * wide, 3 * wide), BF16),
            pltpu.VMEM((groups, 4, (nframe + 2) * ncol, cl), BF16),
            pltpu.VMEM((3, 2 * pos, width), F32),
            pltpu.VMEM((9 * pos, pos), BF16),
            pltpu.VMEM((groups, wide // groups, pos), F32),
            pltpu.VMEM((groups, wide // groups, pos), F32),
            pltpu.VMEM((count, groups, wide // groups, pos), BF16),
            pltpu.SemaphoreType.REGULAR((count.bit_length() - 1,)),
            dma((5,)),
            dma((3,)),
            dma((3 * SPLIT,)),
            dma((3,)),
            dma((2,)),
            dma((2,)),
            dma((groups,)),
            dma((groups,)),
            dma((groups, 2)),
            dma((groups, 2)),
            dma((groups,)),
            dma((groups,)),
            dma((count,)),
            dma((count,)),
            dma((groups,)),
            dma((groups,)),
            dma((share,)),
            dma((share,)),
        ],
        compiler_params=pltpu.CompilerParams(
            collective_id=0, has_side_effects=True, vmem_limit_bytes=60 * 1024 * 1024
        ),
    )(
        frames_in,
        conv_weight,
        w2,
        embed_weight.reshape(wide, depth),
        norm_gain.reshape(1, -1),
        q_weight,
        k_weight,
        v_weight,
    )
    own = count * (ncol // 2)
    tokens = count * pos // 2
    shape = jax.ShapeDtypeStruct((own, hw), BF16)
    return pl.pallas_call(
        functools.partial(attend_kernel, count, ncol // 2),
        out_shape=(shape,) * 3,
        in_specs=[ANY_SPEC] * 5,
        out_specs=(ANY_SPEC,) * 3,
        scratch_shapes=[
            pltpu.VMEM((count, wide, pos), BF16),
            pltpu.VMEM((share, 3, wide, quarter), BF16),
            pltpu.VMEM(((heads + 1) * wide, 3 * wide), BF16),
            pltpu.VMEM((1, hsize), F32),
            pltpu.VMEM((1, hsize), F32),
            pltpu.VMEM((own, hw), BF16),
            pltpu.VMEM((own, hw), BF16),
            pltpu.VMEM((own, hw), BF16),
            pltpu.VMEM((3 * wide + 16, tokens), BF16),
            pltpu.VMEM((wide, tokens), F32),
            pltpu.VMEM((wide, tokens), BF16),
            pltpu.VMEM((heads + 1, tokens), F32),
            pltpu.VMEM((heads, tokens), F32),
            pltpu.VMEM((heads, own, 3 * wide + 16), BF16),
            dma((5,)),
            dma((3,)),
        ],
        compiler_params=pltpu.CompilerParams(vmem_limit_bytes=67043328),
    )(
        gath.reshape(count, wide, pos),
        m,
        gram,
        q_gain.reshape(1, -1),
        k_gain.reshape(1, -1),
    )


def solution(mesh):
    in_specs = (
        P(None, "sp", None, "hd"),
        P(None, None, None, None, "hd"),
        P(None, None, None, "hd", None),
        P(),
        P(),
        P(None, "hd"),
        P(None, "hd"),
        P(None, "hd"),
        P(),
        P(),
    )
    out_specs = (P("sp", "hd"), P("sp", "hd"), P("sp", "hd"))
    return jax.shard_map(
        on_device, mesh=mesh, in_specs=in_specs, out_specs=out_specs, check_vma=False
    )
```

```python
import functools
import math

import jax
import jax.numpy as jnp
from jax import lax
from jax.experimental import pallas as pl
from jax.experimental.pallas import tpu as pltpu
from jax.sharding import PartitionSpec as P

EPS = 1e-06
MESH = pl.DeviceIdType.MESH
ANY_SPEC = pl.BlockSpec(memory_space=pl.ANY)
VMEM_SPEC = pl.BlockSpec(memory_space=pltpu.VMEM)
SPLIT = 1
F32 = jnp.float32
BF16 = jnp.bfloat16


def dot_nt(a, b):
    return lax.dot_general(a, b, (((1,), (1,)), ((), ())), preferred_element_type=F32)


def dot(a, b):
    return jnp.dot(a, b, preferred_element_type=F32)


def encode_kernel(
    count,
    groups,
    share,
    x_ref,
    cw_ref,
    w2_ref,
    emb_ref,
    gain_ref,
    wq_ref,
    wk_ref,
    wv_ref,
    gath_out,
    m_out,
    gram_out,
    land,
    cwv,
    w2v,
    embv,
    gainv,
    wbuf,
    eb,
    mbuf,
    grambuf,
    xs,
    acc,
    shift,
    pown,
    pin,
    gbuf,
    ready,
    in_sem,
    cw_sem,
    w_sem,
    out_sem,
    halo_send,
    halo_recv,
    own_send,
    own_recv,
    fwd_send,
    fwd_recv,
    part_send,
    part_recv,
    gath_send,
    gath_recv,
    relay_send,
    relay_recv,
    m_send,
    m_recv,
):
    sp, hd = lax.axis_index("sp"), lax.axis_index("hd")
    nframe, ncol, cl = land.shape[2:]
    pos = nframe * ncol
    depth = eb.shape[1]
    step_rows = depth // SPLIT
    lat = w2v.shape[3]
    bits = count.bit_length() - 1
    first, last = sp == 0, sp == count - 1

    rows_in = [
        pltpu.make_async_copy(x_ref.at[:, r], land.at[hd, 1 + r], in_sem.at[r]) for r in range(2)
    ]
    emb_in = pltpu.make_async_copy(emb_ref, embv, in_sem.at[2])
    gain_in = pltpu.make_async_copy(gain_ref, gainv, in_sem.at[3])
    w2_in = pltpu.make_async_copy(w2_ref, w2v, in_sem.at[4])
    cw_in = [
        pltpu.make_async_copy(cw_ref.at[:, dh], cwv.at[:, dh], cw_sem.at[dh]) for dh in range(3)
    ]

    slot = sp % share
    quarter = wbuf.shape[2]

    def w_in(i):
        w, part = divmod(i, SPLIT)
        at = pl.ds(part * step_rows, step_rows)
        cols = pl.ds(pl.multiple_of(slot * quarter, quarter), quarter)
        ref = (wq_ref, wk_ref, wv_ref)[w]
        return pltpu.make_async_copy(
            ref.at[at] if share == 1 else ref.at[at, cols], wbuf.at[w, at], w_sem.at[i]
        )

    for copy in rows_in + [emb_in, gain_in]:
        copy.start()
    for i in range(3 * SPLIT):
        w_in(i).start()
    barrier = pltpu.get_barrier_semaphore()
    prev_id, next_id = (jnp.maximum(sp - 1, 0), hd), (jnp.minimum(sp + 1, count - 1), hd)

    def across(k):
        low = sp % (2 * k)
        return (jnp.where(low >= k, sp - k, sp + k), hd)

    def arrive(device):
        pl.semaphore_signal(barrier, inc=1, device_id=device, device_id_type=MESH)

    @pl.when(jnp.logical_not(first))
    def _():
        arrive(prev_id)

    @pl.when(jnp.logical_not(last))
    def _():
        arrive(next_id)

    for bit in range(bits):
        arrive(across(1 << bit))
    for k in range(1, groups):
        arrive((sp, lax.rem(hd + k, groups)))

    def mate(k):
        return (sp, lax.rem(hd + k, groups))

    def remote(src, dst, send, recv, device):
        return pltpu.make_async_remote_copy(
            src_ref=src,
            dst_ref=dst,
            send_sem=send,
            recv_sem=recv,
            device_id=device,
            device_id_type=MESH,
        )

    def flip(k):
        other = sp
        for bit in range(bits):
            if (k >> bit) & 1:
                low = sp % (2 << bit)
                other = other + jnp.where(low >= (1 << bit), -(1 << bit), 1 << bit)
        return other

    def tell(bit):
        pl.semaphore_signal(
            ready.at[bit], inc=1, device_id=across(1 << bit), device_id_type=MESH
        )

    def hear(bit):
        pl.semaphore_wait(ready.at[bit], 1)

    for copy in rows_in:
        copy.wait()
    ends = jnp.where(first, 0, 1) + jnp.where(last, 0, 1)
    pl.semaphore_wait(barrier, bits + groups - 1 + ends)

    to_prev = remote(
        land.at[hd, 1], land.at[hd, 3], halo_send.at[0], halo_recv.at[0], prev_id
    )
    to_next = remote(
        land.at[hd, 2], land.at[hd, 0], halo_send.at[1], halo_recv.at[1], next_id
    )

    @pl.when(jnp.logical_not(first))
    def _():
        to_prev.start()

    @pl.when(jnp.logical_not(last))
    def _():
        to_next.start()

    own_out = [
        remote(
            land.at[hd, pl.ds(1, 2)],
            land.at[hd, pl.ds(1, 2)],
            own_send.at[k],
            own_recv.at[k],
            mate(k),
        )
        for k in range(1, groups)
    ]
    for copy in own_out:
        copy.start()

    tell(0)
    emb_in.wait()
    gain_in.wait()
    ordered = [
        embv[(a * 2 + b) * lat : (a * 2 + b + 1) * lat] for b in range(2) for a in range(2)
    ]
    for i, rows in enumerate(ordered):
        eb[i * lat : (i + 1) * lat] = (rows.astype(F32) * gainv[...]).astype(BF16)
    wide = eb.shape[0]

    def split3(value):
        lane = lax.broadcasted_iota(jnp.int32, value.shape, 1)
        top = value.astype(BF16).astype(F32)
        rest = value - top
        mid = rest.astype(BF16).astype(F32)
        low = rest - mid
        return jnp.where(lane < wide, top, jnp.where(lane < 2 * wide, mid, low)).astype(BF16)

    def gram_of(rows, size):
        return split3(dot_nt(rows, jnp.concatenate([rows] * 3, axis=0)) * (1.0 / size))


    def m_step(i):
        w_in(i).wait()
        if i < 3:
            cw_in[(1, 2, 0)[i]].start()
        if i == 2:
            w2_in.start()
        mbuf[slot, i] = dot(eb[...], wbuf[i]).astype(BF16)

    for i in range(3 * SPLIT):
        m_step(i)
    hear(0)
    tell(1)
    spread_m = [
        remote(mbuf.at[slot], mbuf.at[slot], m_send.at[k], m_recv.at[k], (flip(k), hd))
        for k in range(1, share)
    ]
    for copy in spread_m:
        copy.start()

    def settle(g, r):
        flat = land[g, r].astype(F32).reshape(pos, cl)
        xs[g, r, 2 * ncol :] = flat.astype(BF16)

    for copy in own_out:
        copy.wait_recv()
    for g in range(groups):
        settle(g, 1)
        settle(g, 2)

    def taps(rows, dh, dw, which=range(groups)):
        total = None
        for g in which:
            at = g * cl if isinstance(g, int) else pl.multiple_of(g * cl, cl)
            for dt in range(3):
                window = [xs[g, r, dt * ncol : dt * ncol + pos] for r in rows]
                value = dot(
                    window[0] if len(rows) == 1 else jnp.concatenate(window, axis=0),
                    cwv[dt, dh, dw, pl.ds(at, cl)],
                )
                total = value if total is None else total + value
        return total

    def step_on(bit):
        if bit < bits:
            hear(bit)
        if bit + 1 < bits:
            tell(bit + 1)

    step_on(1)
    for dh in (1, 2, 0):
        cw_in[dh].wait()
    half = pos // 2
    pcol = ncol // 2
    src = lax.broadcasted_iota(jnp.int32, (pos, pos), 0)
    dst = lax.broadcasted_iota(jnp.int32, (pos, pos), 1)
    odd = dst // half
    frame = (dst % half) // pcol
    column = 2 * (dst % pcol) + odd
    for dt in range(3):
        for dw in range(3):
            c = column + (dw - 1)
            hit = (src == (frame + (dt - 2)) * ncol + c) & (c >= 0) & (c < ncol)
            k = dt * 3 + dw
            shift[k * pos : (k + 1) * pos] = jnp.where(hit, 1.0, 0.0).astype(BF16)
    for g in range(groups):
        for r in range(4):
            xs[g, r, 0 : 2 * ncol] = jnp.zeros((2 * ncol, cl), BF16)

    for dw in range(3):
        both = taps((1, 2), 1, dw)
        acc[dw, 0:pos] = both[:pos] + taps((2,), 2, dw)
        acc[dw, pos : 2 * pos] = both[pos:] + taps((1,), 0, dw)
    step_on(2)

    fwd = [
        [
            remote(
                land.at[hd, r],
                land.at[hd, r],
                fwd_send.at[k, r // 3],
                fwd_recv.at[k, r // 3],
                mate(k),
            )
            for k in range(1, groups)
        ]
        for r in (0, 3)
    ]

    @pl.when(jnp.logical_not(first))
    def _():
        to_next.wait_recv()
        for copy in fwd[0]:
            copy.start()
        settle(hd, 0)

    @pl.when(jnp.logical_not(last))
    def _():
        to_prev.wait_recv()
        for copy in fwd[1]:
            copy.start()
        settle(hd, 3)

    @pl.when(first)
    def _():
        for g in range(groups):
            xs[g, 0, 2 * ncol :] = jnp.zeros((pos, cl), BF16)

    @pl.when(last)
    def _():
        for g in range(groups):
            xs[g, 3, 2 * ncol :] = jnp.zeros((pos, cl), BF16)

    def rim_taps(which):
        for dw in range(3):
            acc[dw, 0:pos] += taps((0,), 0, dw, which)
            acc[dw, pos : 2 * pos] += taps((3,), 2, dw, which)

    others = [lax.rem(hd + k, groups) for k in range(1, groups)]
    rim_taps([hd])
    for bit in range(3, bits):
        step_on(bit)

    @pl.when(jnp.logical_not(first))
    def _():
        for copy in fwd[0]:
            copy.wait_recv()
        for g in others:
            settle(g, 0)

    @pl.when(jnp.logical_not(last))
    def _():
        for copy in fwd[1]:
            copy.wait_recv()
        for g in others:
            settle(g, 3)

    rim_taps(others)
    summed = [acc[dw] for dw in range(3)]
    width = summed[0].shape[-1]
    cube = (2 * nframe, ncol, width)
    place = lax.broadcasted_iota(jnp.int32, cube, 1)
    left, middle, right = [value.reshape(cube) for value in summed]
    feature = (
        middle
        + jnp.where(place > 0, pltpu.roll(left, 1, 1), 0.0)
        + jnp.where(place < ncol - 1, pltpu.roll(right, ncol - 1, 1), 0.0)
    )
    feature = jax.nn.silu(feature).reshape(2 * pos, width).astype(BF16)
    w2_in.wait()
    z = dot_nt(w2v[...].reshape(27 * lat, width), feature)

    def piece(dt, dh, dw, f):
        at = ((dt * 3 + dh) * 3 + dw) * lat
        return z[at : at + lat, f * pos : (f + 1) * pos]

    spread = []
    for dt in range(3):
        for dw in range(3):
            spread.append(
                jnp.concatenate(
                    [
                        piece(dt, 2, dw, 0),
                        piece(dt, 1, dw, 0) + piece(dt, 2, dw, 1),
                        piece(dt, 0, dw, 0) + piece(dt, 1, dw, 1),
                        piece(dt, 0, dw, 1),
                    ],
                    axis=0,
                )
            )
    spread = jnp.concatenate(spread, axis=1)
    high = spread.astype(BF16)
    low = (spread - high.astype(F32)).astype(BF16)
    moved = dot(high, shift[...]) + dot(low, shift[...])
    pown[...] = moved.reshape(pown.shape)

    parts = [
        remote(
            pown.at[lax.rem(hd + k, groups)],
            pin.at[k],
            part_send.at[k],
            part_recv.at[k],
            mate(k),
        )
        for k in range(1, groups)
    ]
    for copy in parts:
        copy.start()
    total = pown[hd]
    for k in range(1, groups):
        parts[k - 1].wait_recv()
        total = total + pin[k]
    gbuf[sp, hd] = total.astype(BF16)

    gather = [
        remote(
            gbuf.at[sp, hd],
            gbuf.at[sp, hd],
            gath_send.at[k],
            gath_recv.at[k],
            (flip(k), hd),
        )
        for k in range(count - 1, 0, -1)
    ]
    for copy in gather:
        copy.start()

    embed = [embv[(a * 2 + b) * lat : (a * 2 + b + 1) * lat] for b in range(2) for a in range(2)]
    grambuf[0:wide] = gram_of(jnp.concatenate(embed, axis=0), depth)
    for copy in spread_m:
        copy.wait_recv()
    blocks = grambuf.shape[0] // wide - 1
    per = blocks // share
    hsize = quarter // per
    for h in range(blocks):
        cols = slice((h % per) * hsize, (h % per + 1) * hsize)
        rows = mbuf[h // per, 1, :, cols]
        grambuf[(h + 1) * wide : (h + 2) * wide] = gram_of(rows, hsize)
    outs = [
        pltpu.make_async_copy(mbuf, m_out, out_sem.at[0]),
        pltpu.make_async_copy(grambuf, gram_out, out_sem.at[1]),
    ]
    for copy in outs:
        copy.start()

    for copy in gather:
        copy.wait_recv()
    relay = [
        remote(gbuf.at[:, hd], gath_out.at[:, hd], relay_send.at[k], relay_recv.at[k], mate(k))
        for k in range(1, groups)
    ]
    for copy in relay:
        copy.start()
    result = pltpu.make_async_copy(gbuf.at[:, hd], gath_out.at[:, hd], out_sem.at[2])
    result.start()
    for copy in relay:
        copy.wait_recv()

    @pl.when(jnp.logical_not(first))
    def _():
        to_prev.wait_send()
        for copy in fwd[0]:
            copy.wait_send()

    @pl.when(jnp.logical_not(last))
    def _():
        to_next.wait_send()
        for copy in fwd[1]:
            copy.wait_send()

    for copy in own_out + spread_m + parts + gather + relay:
        copy.wait_send()
    for copy in outs:
        copy.wait()
    result.wait()


def attend_kernel(
    count,
    pcol,
    gath_hbm,
    m_hbm,
    gram_hbm,
    qg_hbm,
    kg_hbm,
    att_hbm,
    key_hbm,
    val_hbm,
    gath_ref,
    m_ref,
    gram_ref,
    qg_ref,
    kg_ref,
    att_ref,
    key_ref,
    val_ref,
    pt,
    pf,
    pn,
    norm,
    factor,
    left,
    in_sem,
    out_sem,
):
    sp = lax.axis_index("sp")
    loads = [
        pltpu.make_async_copy(src, dst, in_sem.at[i])
        for i, (src, dst) in enumerate(
            (
                (gath_hbm, gath_ref),
                (qg_hbm, qg_ref),
                (kg_hbm, kg_ref),
                (m_hbm, m_ref),
                (gram_hbm, gram_ref),
            )
        )
    ]
    for copy in loads:
        copy.start()
    lanes = gath_ref.shape[2]
    half = lanes // 2
    lat = gath_ref.shape[1] // 4
    wide = 4 * lat
    tokens = count * half
    own = count * pcol
    hsize = qg_ref.shape[1]
    share = m_ref.shape[0]
    per = m_ref.shape[3] // hsize
    heads = share * per
    pair = 4 if heads % 4 == 0 else 1
    deep = pt.shape[0]

    row = lax.broadcasted_iota(jnp.int32, (own, tokens), 0)
    lane = lax.broadcasted_iota(jnp.int32, (own, tokens), 1)
    want = (row // pcol) * half + sp * pcol + row % pcol
    pick = jnp.where(lane == want, 1.0, 0.0).astype(BF16)
    tail = (deep - 3 * wide, tokens)
    frame = (lax.broadcasted_iota(jnp.int32, tail, 1) % half) // pcol
    hidden = (frame > sp) & (lax.broadcasted_iota(jnp.int32, tail, 0) == 0)
    pt[3 * wide : deep] = jnp.where(hidden, -1e30, 0.0).astype(BF16)
    rest = (own, deep - 2 * wide)
    ones = jnp.where(lax.broadcasted_iota(jnp.int32, rest, 1) == wide, 1.0, 0.0).astype(BF16)
    for h in range(heads):
        left[h, :, 2 * wide : deep] = ones

    def level(r, a):
        value = gath_ref[r, (1 + a) * lat : (2 + a) * lat].astype(F32)
        if a == 0 and r > 0:
            value = value + gath_ref[r - 1, 3 * lat : 4 * lat].astype(F32)
        if a == 1 and r < count - 1:
            value = value + gath_ref[r + 1, 0:lat].astype(F32)
        return value

    loads[0].wait()
    joint = max(1, 128 // half)
    for r in range(0, count, joint):
        rows = [jnp.concatenate([level(r + j, 0), level(r + j, 1)], axis=0) for j in range(joint)]
        if joint == 1:
            even, odds = rows[0][:, :half], rows[0][:, half:]
        else:
            turn = lax.broadcasted_iota(jnp.int32, rows[0].shape, 1)
            even = jnp.where(turn < half, rows[0], pltpu.roll(rows[1], half, 1))
            odds = jnp.where(turn < half, pltpu.roll(rows[0], half, 1), rows[1])
        block = jnp.concatenate([even, odds], axis=0).astype(BF16)
        at = slice(r * half, (r + joint) * half)
        for i in range(3):
            pt[i * wide : (i + 1) * wide, at] = block
        pf[:, at] = block.astype(F32)

    patches = pt[0:wide]
    mine16 = dot_nt(pick, patches).astype(BF16)
    for copy in loads[1:]:
        copy.wait()

    span = min(tokens, 256)
    for at in range(0, tokens, span):
        cols = slice(at, at + span)
        spread = dot(gram_ref[...], pt[0 : 3 * wide, cols]).reshape(heads + 1, wide, span)
        norm[:, cols] = jnp.maximum(jnp.sum(spread * pf[:, cols][None], axis=1), 0.0)
    rs = lax.rsqrt(norm[0:1] + EPS)
    own_rs = jnp.sum(jnp.where(lane == want, rs, 0.0), axis=1, keepdims=True)

    def project(w):
        parts = [dot(mine16, m_ref[i, w]) for i in range(share)]
        return jnp.concatenate(parts, axis=1) * own_rs

    def matrix(w, h):
        return m_ref[h // per, w, :, (h % per) * hsize : (h % per + 1) * hsize]

    val_ref[...] = project(2).astype(BF16)
    raw_k = project(1)
    raw_q = project(0)
    pn[...] = (pf[...] * rs).astype(BF16)
    scale = hsize ** (-0.5) * math.log2(math.e)

    def unit(value):
        return value * lax.rsqrt(jnp.mean(value * value, axis=1, keepdims=True) + EPS)

    side = lax.broadcasted_iota(jnp.int32, (own, 2 * wide), 1)
    for h in range(heads):
        cols = slice(h * hsize, (h + 1) * hsize)
        key_ref[:, cols] = (unit(raw_k[:, cols]) * kg_ref[...]).astype(BF16)
        q = (unit(raw_q[:, cols]) * qg_ref[...] * (kg_ref[...] * scale)).astype(BF16)
        mk = matrix(1, h)
        narrow = dot_nt(q, jnp.concatenate([mk, mk], axis=0))
        top = narrow.astype(BF16).astype(F32)
        left[h, :, 0 : 2 * wide] = jnp.where(side < wide, top, narrow - top).astype(BF16)
    early = [
        pltpu.make_async_copy(key_ref, key_hbm, out_sem.at[0]),
        pltpu.make_async_copy(val_ref, val_hbm, out_sem.at[1]),
    ]
    for copy in early:
        copy.start()
    factor[...] = rs * lax.rsqrt(rs * rs * norm[1 : heads + 1] + EPS)

    def score(step):
        rows = left[step * pair : (step + 1) * pair].reshape(pair * own, deep)
        return dot(rows, pt[...])

    ahead = score(0)
    for step in range(heads // pair):
        scores = ahead
        if step + 1 < heads // pair:
            ahead = score(step + 1)
        soft, totals = [], []
        for j in range(pair):
            h = step * pair + j
            part = scores[j * own : (j + 1) * own] * factor[h : h + 1]
            peak = jnp.max(part, axis=1, keepdims=True)
            weights = jnp.exp2(part - peak)
            totals.append(jnp.sum(weights, axis=1, keepdims=True))
            soft.append(weights.astype(BF16))
        mixed = dot_nt(jnp.concatenate(soft, axis=0), pn[...]).astype(BF16)
        for j in range(pair):
            h = step * pair + j
            cols = slice(h * hsize, (h + 1) * hsize)
            out = dot(mixed[j * own : (j + 1) * own], matrix(2, h))
            att_ref[:, cols] = (out / totals[j]).astype(BF16)

    late = pltpu.make_async_copy(att_ref, att_hbm, out_sem.at[2])
    late.start()
    for copy in early + [late]:
        copy.wait()


def on_device(
    frames_in,
    conv_weight,
    conv_out_weight,
    embed_weight,
    norm_gain,
    q_weight,
    k_weight,
    v_weight,
    q_gain,
    k_gain,
):
    count, groups = lax.axis_size("sp"), lax.axis_size("hd")
    nframe, own_rows, ncol, cl = frames_in.shape
    if own_rows != 2 or nframe != count or count & (count - 1):
        raise ValueError("unsupported shape")
    cin, width = conv_weight.shape[-2:]
    lat = conv_out_weight.shape[-1]
    wide = 4 * lat
    depth, hw = q_weight.shape
    pos = nframe * ncol
    hsize = q_gain.shape[0]
    w2 = conv_out_weight.transpose(0, 1, 2, 4, 3)
    dma = pltpu.SemaphoreType.DMA
    heads = hw // hsize
    share = 4 if heads % 4 == 0 and count >= 4 else 1
    quarter = hw // share
    gath, m, gram = pl.pallas_call(
        functools.partial(encode_kernel, count, groups, share),
        out_shape=(
            jax.ShapeDtypeStruct((count, groups, wide // groups, pos), BF16),
            jax.ShapeDtypeStruct((share, 3, wide, quarter), BF16),
            jax.ShapeDtypeStruct(((hw // hsize + 1) * wide, 3 * wide), BF16),
        ),
        in_specs=[ANY_SPEC] * 8,
        out_specs=(ANY_SPEC,) * 3,
        scratch_shapes=[
            pltpu.VMEM((groups, 4, nframe, ncol, cl), BF16),
            pltpu.VMEM((3, 3, 3, cin, width), BF16),
            pltpu.VMEM((3, 3, 3, lat, width), BF16),
            pltpu.VMEM((wide, depth), BF16),
            pltpu.VMEM((1, depth), F32),
            pltpu.VMEM((3, depth, quarter), BF16),
            pltpu.VMEM((wide, depth), BF16),
            pltpu.VMEM((share, 3, wide, quarter), BF16),
            pltpu.VMEM(((hw // hsize + 1) * wide, 3 * wide), BF16),
            pltpu.VMEM((groups, 4, (nframe + 2) * ncol, cl), BF16),
            pltpu.VMEM((3, 2 * pos, width), F32),
            pltpu.VMEM((9 * pos, pos), BF16),
            pltpu.VMEM((groups, wide // groups, pos), F32),
            pltpu.VMEM((groups, wide // groups, pos), F32),
            pltpu.VMEM((count, groups, wide // groups, pos), BF16),
            pltpu.SemaphoreType.REGULAR((count.bit_length() - 1,)),
            dma((5,)),
            dma((3,)),
            dma((3 * SPLIT,)),
            dma((3,)),
            dma((2,)),
            dma((2,)),
            dma((groups,)),
            dma((groups,)),
            dma((groups, 2)),
            dma((groups, 2)),
            dma((groups,)),
            dma((groups,)),
            dma((count,)),
            dma((count,)),
            dma((groups,)),
            dma((groups,)),
            dma((share,)),
            dma((share,)),
        ],
        compiler_params=pltpu.CompilerParams(
            collective_id=0, has_side_effects=True, vmem_limit_bytes=60 * 1024 * 1024
        ),
    )(
        frames_in,
        conv_weight,
        w2,
        embed_weight.reshape(wide, depth),
        norm_gain.reshape(1, -1),
        q_weight,
        k_weight,
        v_weight,
    )
    own = count * (ncol // 2)
    tokens = count * pos // 2
    shape = jax.ShapeDtypeStruct((own, hw), BF16)
    return pl.pallas_call(
        functools.partial(attend_kernel, count, ncol // 2),
        out_shape=(shape,) * 3,
        in_specs=[ANY_SPEC] * 5,
        out_specs=(ANY_SPEC,) * 3,
        scratch_shapes=[
            pltpu.VMEM((count, wide, pos), BF16),
            pltpu.VMEM((share, 3, wide, quarter), BF16),
            pltpu.VMEM(((heads + 1) * wide, 3 * wide), BF16),
            pltpu.VMEM((1, hsize), F32),
            pltpu.VMEM((1, hsize), F32),
            pltpu.VMEM((own, hw), BF16),
            pltpu.VMEM((own, hw), BF16),
            pltpu.VMEM((own, hw), BF16),
            pltpu.VMEM((3 * wide + 16, tokens), BF16),
            pltpu.VMEM((wide, tokens), F32),
            pltpu.VMEM((wide, tokens), BF16),
            pltpu.VMEM((heads + 1, tokens), F32),
            pltpu.VMEM((heads, tokens), F32),
            pltpu.VMEM((heads, own, 3 * wide + 16), BF16),
            dma((5,)),
            dma((3,)),
        ],
        compiler_params=pltpu.CompilerParams(vmem_limit_bytes=67043328),
    )(
        gath.reshape(count, wide, pos),
        m,
        gram,
        q_gain.reshape(1, -1),
        k_gain.reshape(1, -1),
    )


def solution(mesh):
    in_specs = (
        P(None, "sp", None, "hd"),
        P(None, None, None, None, "hd"),
        P(None, None, None, "hd", None),
        P(),
        P(),
        P(None, "hd"),
        P(None, "hd"),
        P(None, "hd"),
        P(),
        P(),
    )
    out_specs = (P("sp", "hd"), P("sp", "hd"), P("sp", "hd"))
    return jax.shard_map(
        on_device, mesh=mesh, in_specs=in_specs, out_specs=out_specs, check_vma=False
    )
```

```python
import functools
import math

import jax
import jax.numpy as jnp
from jax import lax
from jax.experimental import pallas as pl
from jax.experimental.pallas import tpu as pltpu
from jax.sharding import PartitionSpec as P

EPS = 1e-06
MESH = pl.DeviceIdType.MESH
ANY_SPEC = pl.BlockSpec(memory_space=pl.ANY)
VMEM_SPEC = pl.BlockSpec(memory_space=pltpu.VMEM)
SPLIT = 1
F32 = jnp.float32
BF16 = jnp.bfloat16


def dot_nt(a, b):
    return lax.dot_general(a, b, (((1,), (1,)), ((), ())), preferred_element_type=F32)


def dot(a, b):
    return jnp.dot(a, b, preferred_element_type=F32)


def encode_kernel(
    count,
    groups,
    share,
    x_ref,
    cw_ref,
    w2_ref,
    emb_ref,
    gain_ref,
    wq_ref,
    wk_ref,
    wv_ref,
    gath_out,
    m_out,
    gram_out,
    land,
    cwv,
    w2v,
    embv,
    gainv,
    wbuf,
    eb,
    mbuf,
    grambuf,
    xs,
    acc,
    shift,
    pown,
    pin,
    gbuf,
    ready,
    in_sem,
    cw_sem,
    w_sem,
    out_sem,
    halo_send,
    halo_recv,
    own_send,
    own_recv,
    fwd_send,
    fwd_recv,
    part_send,
    part_recv,
    gath_send,
    gath_recv,
    relay_send,
    relay_recv,
    m_send,
    m_recv,
):
    sp, hd = lax.axis_index("sp"), lax.axis_index("hd")
    nframe, ncol, cl = land.shape[2:]
    pos = nframe * ncol
    depth = eb.shape[1]
    step_rows = depth // SPLIT
    lat = w2v.shape[3]
    bits = count.bit_length() - 1
    first, last = sp == 0, sp == count - 1

    rows_in = [
        pltpu.make_async_copy(x_ref.at[:, r], land.at[hd, 1 + r], in_sem.at[r]) for r in range(2)
    ]
    emb_in = pltpu.make_async_copy(emb_ref, embv, in_sem.at[2])
    gain_in = pltpu.make_async_copy(gain_ref, gainv, in_sem.at[3])
    w2_in = pltpu.make_async_copy(w2_ref, w2v, in_sem.at[4])
    cw_in = [
        pltpu.make_async_copy(cw_ref.at[:, dh], cwv.at[:, dh], cw_sem.at[dh]) for dh in range(3)
    ]

    slot = sp % share
    quarter = wbuf.shape[2]

    def w_in(i):
        w, part = divmod(i, SPLIT)
        at = pl.ds(part * step_rows, step_rows)
        cols = pl.ds(pl.multiple_of(slot * quarter, quarter), quarter)
        ref = (wq_ref, wk_ref, wv_ref)[w]
        return pltpu.make_async_copy(
            ref.at[at] if share == 1 else ref.at[at, cols], wbuf.at[w, at], w_sem.at[i]
        )

    for copy in rows_in + [emb_in, gain_in]:
        copy.start()
    for i in range(3 * SPLIT):
        w_in(i).start()
    cw_in[1].start()
    barrier = pltpu.get_barrier_semaphore()
    prev_id, next_id = (jnp.maximum(sp - 1, 0), hd), (jnp.minimum(sp + 1, count - 1), hd)

    def across(k):
        low = sp % (2 * k)
        return (jnp.where(low >= k, sp - k, sp + k), hd)

    def arrive(device):
        pl.semaphore_signal(barrier, inc=1, device_id=device, device_id_type=MESH)

    @pl.when(jnp.logical_not(first))
    def _():
        arrive(prev_id)

    @pl.when(jnp.logical_not(last))
    def _():
        arrive(next_id)

    for bit in range(bits):
        arrive(across(1 << bit))
    for k in range(1, groups):
        arrive((sp, lax.rem(hd + k, groups)))

    def mate(k):
        return (sp, lax.rem(hd + k, groups))

    def remote(src, dst, send, recv, device):
        return pltpu.make_async_remote_copy(
            src_ref=src,
            dst_ref=dst,
            send_sem=send,
            recv_sem=recv,
            device_id=device,
            device_id_type=MESH,
        )

    def flip(k):
        other = sp
        for bit in range(bits):
            if (k >> bit) & 1:
                low = sp % (2 << bit)
                other = other + jnp.where(low >= (1 << bit), -(1 << bit), 1 << bit)
        return other

    def tell(bit):
        pl.semaphore_signal(
            ready.at[bit], inc=1, device_id=across(1 << bit), device_id_type=MESH
        )

    def hear(bit):
        pl.semaphore_wait(ready.at[bit], 1)

    for copy in rows_in:
        copy.wait()
    ends = jnp.where(first, 0, 1) + jnp.where(last, 0, 1)
    pl.semaphore_wait(barrier, bits + groups - 1 + ends)

    to_prev = remote(
        land.at[hd, 1], land.at[hd, 3], halo_send.at[0], halo_recv.at[0], prev_id
    )
    to_next = remote(
        land.at[hd, 2], land.at[hd, 0], halo_send.at[1], halo_recv.at[1], next_id
    )

    @pl.when(jnp.logical_not(first))
    def _():
        to_prev.start()

    @pl.when(jnp.logical_not(last))
    def _():
        to_next.start()

    own_out = [
        remote(
            land.at[hd, pl.ds(1, 2)],
            land.at[hd, pl.ds(1, 2)],
            own_send.at[k],
            own_recv.at[k],
            mate(k),
        )
        for k in range(1, groups)
    ]
    for copy in own_out:
        copy.start()

    tell(0)
    emb_in.wait()
    gain_in.wait()
    ordered = [
        embv[(a * 2 + b) * lat : (a * 2 + b + 1) * lat] for b in range(2) for a in range(2)
    ]
    for i, rows in enumerate(ordered):
        eb[i * lat : (i + 1) * lat] = (rows.astype(F32) * gainv[...]).astype(BF16)
    wide = eb.shape[0]

    def split3(value):
        lane = lax.broadcasted_iota(jnp.int32, value.shape, 1)
        top = value.astype(BF16).astype(F32)
        rest = value - top
        mid = rest.astype(BF16).astype(F32)
        low = rest - mid
        return jnp.where(lane < wide, top, jnp.where(lane < 2 * wide, mid, low)).astype(BF16)

    def gram_of(rows, size):
        return split3(dot_nt(rows, jnp.concatenate([rows] * 3, axis=0)) * (1.0 / size))


    def m_step(i):
        w_in(i).wait()
        if i == 0:
            for dh in (2, 0):
                cw_in[dh].start()
            w2_in.start()
        mbuf[slot, i] = dot(eb[...], wbuf[i]).astype(BF16)

    for i in range(3 * SPLIT):
        m_step(i)
    hear(0)
    tell(1)
    spread_m = [
        remote(mbuf.at[slot], mbuf.at[slot], m_send.at[k], m_recv.at[k], (flip(k), hd))
        for k in range(1, share)
    ]
    for copy in spread_m:
        copy.start()

    def settle(g, r):
        flat = land[g, r].astype(F32).reshape(pos, cl)
        xs[g, r, 2 * ncol :] = flat.astype(BF16)

    for copy in own_out:
        copy.wait_recv()
    for g in range(groups):
        settle(g, 1)
        settle(g, 2)

    def taps(rows, dh, dw, which=range(groups)):
        total = None
        for g in which:
            at = g * cl if isinstance(g, int) else pl.multiple_of(g * cl, cl)
            for dt in range(3):
                window = [xs[g, r, dt * ncol : dt * ncol + pos] for r in rows]
                value = dot(
                    window[0] if len(rows) == 1 else jnp.concatenate(window, axis=0),
                    cwv[dt, dh, dw, pl.ds(at, cl)],
                )
                total = value if total is None else total + value
        return total

    def step_on(bit):
        if bit < bits:
            hear(bit)
        if bit + 1 < bits:
            tell(bit + 1)

    step_on(1)
    for dh in (1, 2, 0):
        cw_in[dh].wait()
    half = pos // 2
    pcol = ncol // 2
    src = lax.broadcasted_iota(jnp.int32, (pos, pos), 0)
    dst = lax.broadcasted_iota(jnp.int32, (pos, pos), 1)
    odd = dst // half
    frame = (dst % half) // pcol
    column = 2 * (dst % pcol) + odd
    for dt in range(3):
        for dw in range(3):
            c = column + (dw - 1)
            hit = (src == (frame + (dt - 2)) * ncol + c) & (c >= 0) & (c < ncol)
            k = dt * 3 + dw
            shift[k * pos : (k + 1) * pos] = jnp.where(hit, 1.0, 0.0).astype(BF16)
    for g in range(groups):
        for r in range(4):
            xs[g, r, 0 : 2 * ncol] = jnp.zeros((2 * ncol, cl), BF16)

    for dw in range(3):
        both = taps((1, 2), 1, dw)
        acc[dw, 0:pos] = both[:pos] + taps((2,), 2, dw)
        acc[dw, pos : 2 * pos] = both[pos:] + taps((1,), 0, dw)
    step_on(2)

    fwd = [
        [
            remote(
                land.at[hd, r],
                land.at[hd, r],
                fwd_send.at[k, r // 3],
                fwd_recv.at[k, r // 3],
                mate(k),
            )
            for k in range(1, groups)
        ]
        for r in (0, 3)
    ]

    @pl.when(jnp.logical_not(first))
    def _():
        to_next.wait_recv()
        for copy in fwd[0]:
            copy.start()
        settle(hd, 0)

    @pl.when(jnp.logical_not(last))
    def _():
        to_prev.wait_recv()
        for copy in fwd[1]:
            copy.start()
        settle(hd, 3)

    @pl.when(first)
    def _():
        for g in range(groups):
            xs[g, 0, 2 * ncol :] = jnp.zeros((pos, cl), BF16)

    @pl.when(last)
    def _():
        for g in range(groups):
            xs[g, 3, 2 * ncol :] = jnp.zeros((pos, cl), BF16)

    def rim_taps(which):
        for dw in range(3):
            acc[dw, 0:pos] += taps((0,), 0, dw, which)
            acc[dw, pos : 2 * pos] += taps((3,), 2, dw, which)

    others = [lax.rem(hd + k, groups) for k in range(1, groups)]
    rim_taps([hd])
    for bit in range(3, bits):
        step_on(bit)

    @pl.when(jnp.logical_not(first))
    def _():
        for copy in fwd[0]:
            copy.wait_recv()
        for g in others:
            settle(g, 0)

    @pl.when(jnp.logical_not(last))
    def _():
        for copy in fwd[1]:
            copy.wait_recv()
        for g in others:
            settle(g, 3)

    summed = []
    for dw in range(3):
        upper = acc[dw, 0:pos] + taps((0,), 0, dw, others)
        lower = acc[dw, pos : 2 * pos] + taps((3,), 2, dw, others)
        summed.append(jnp.concatenate([upper, lower], axis=0))
    width = summed[0].shape[-1]
    cube = (2 * nframe, ncol, width)
    place = lax.broadcasted_iota(jnp.int32, cube, 1)
    left, middle, right = [value.reshape(cube) for value in summed]
    feature = (
        middle
        + jnp.where(place > 0, pltpu.roll(left, 1, 1), 0.0)
        + jnp.where(place < ncol - 1, pltpu.roll(right, ncol - 1, 1), 0.0)
    )
    feature = jax.nn.silu(feature).reshape(2 * pos, width).astype(BF16)
    w2_in.wait()
    z = dot_nt(w2v[...].reshape(27 * lat, width), feature)

    def piece(dt, dh, dw, f):
        at = ((dt * 3 + dh) * 3 + dw) * lat
        return z[at : at + lat, f * pos : (f + 1) * pos]

    spread = []
    for dt in range(3):
        for dw in range(3):
            spread.append(
                jnp.concatenate(
                    [
                        piece(dt, 2, dw, 0),
                        piece(dt, 1, dw, 0) + piece(dt, 2, dw, 1),
                        piece(dt, 0, dw, 0) + piece(dt, 1, dw, 1),
                        piece(dt, 0, dw, 1),
                    ],
                    axis=0,
                )
            )
    spread = jnp.concatenate(spread, axis=1)
    high = spread.astype(BF16)
    low = (spread - high.astype(F32)).astype(BF16)
    moved = dot(jnp.concatenate([high, low], axis=0), shift[...])
    moved = moved[:wide] + moved[wide:]
    pown[...] = moved.reshape(pown.shape)

    parts = [
        remote(
            pown.at[lax.rem(hd + k, groups)],
            pin.at[k],
            part_send.at[k],
            part_recv.at[k],
            mate(k),
        )
        for k in range(1, groups)
    ]
    for copy in parts:
        copy.start()
    total = pown[hd]
    for k in range(1, groups):
        parts[k - 1].wait_recv()
        total = total + pin[k]
    gbuf[sp, hd] = total.astype(BF16)

    gather = [
        remote(
            gbuf.at[sp, hd],
            gbuf.at[sp, hd],
            gath_send.at[k],
            gath_recv.at[k],
            (flip(k), hd),
        )
        for k in range(count - 1, 0, -1)
    ]
    for copy in gather:
        copy.start()

    embed = [embv[(a * 2 + b) * lat : (a * 2 + b + 1) * lat] for b in range(2) for a in range(2)]
    grambuf[0:wide] = gram_of(jnp.concatenate(embed, axis=0), depth)
    for copy in spread_m:
        copy.wait_recv()
    blocks = grambuf.shape[0] // wide - 1
    per = blocks // share
    hsize = quarter // per
    for h in range(blocks):
        cols = slice((h % per) * hsize, (h % per + 1) * hsize)
        rows = mbuf[h // per, 1, :, cols]
        grambuf[(h + 1) * wide : (h + 2) * wide] = gram_of(rows, hsize)
    outs = [
        pltpu.make_async_copy(mbuf, m_out, out_sem.at[0]),
        pltpu.make_async_copy(grambuf, gram_out, out_sem.at[1]),
    ]
    for copy in outs:
        copy.start()

    for copy in gather:
        copy.wait_recv()
    relay = [
        remote(gbuf.at[:, hd], gath_out.at[:, hd], relay_send.at[k], relay_recv.at[k], mate(k))
        for k in range(1, groups)
    ]
    for copy in relay:
        copy.start()
    result = pltpu.make_async_copy(gbuf.at[:, hd], gath_out.at[:, hd], out_sem.at[2])
    result.start()
    for copy in relay:
        copy.wait_recv()

    @pl.when(jnp.logical_not(first))
    def _():
        to_prev.wait_send()
        for copy in fwd[0]:
            copy.wait_send()

    @pl.when(jnp.logical_not(last))
    def _():
        to_next.wait_send()
        for copy in fwd[1]:
            copy.wait_send()

    for copy in own_out + spread_m + parts + gather + relay:
        copy.wait_send()
    for copy in outs:
        copy.wait()
    result.wait()


def attend_kernel(
    count,
    pcol,
    gath_hbm,
    m_hbm,
    gram_hbm,
    qg_hbm,
    kg_hbm,
    att_hbm,
    key_hbm,
    val_hbm,
    gath_ref,
    m_ref,
    gram_ref,
    qg_ref,
    kg_ref,
    att_ref,
    key_ref,
    val_ref,
    pt,
    pf,
    pn,
    norm,
    factor,
    left,
    in_sem,
    out_sem,
):
    sp = lax.axis_index("sp")
    loads = [
        pltpu.make_async_copy(src, dst, in_sem.at[i])
        for i, (src, dst) in enumerate(
            (
                (gath_hbm, gath_ref),
                (qg_hbm, qg_ref),
                (kg_hbm, kg_ref),
                (m_hbm, m_ref),
                (gram_hbm, gram_ref),
            )
        )
    ]
    for copy in loads:
        copy.start()
    lanes = gath_ref.shape[2]
    half = lanes // 2
    lat = gath_ref.shape[1] // 4
    wide = 4 * lat
    tokens = count * half
    own = count * pcol
    hsize = qg_ref.shape[1]
    share = m_ref.shape[0]
    per = m_ref.shape[3] // hsize
    heads = share * per
    pair = 4 if heads % 4 == 0 else 1
    deep = pt.shape[0]

    row = lax.broadcasted_iota(jnp.int32, (own, tokens), 0)
    lane = lax.broadcasted_iota(jnp.int32, (own, tokens), 1)
    want = (row // pcol) * half + sp * pcol + row % pcol
    pick = jnp.where(lane == want, 1.0, 0.0).astype(BF16)
    tail = (deep - 3 * wide, tokens)
    frame = (lax.broadcasted_iota(jnp.int32, tail, 1) % half) // pcol
    hidden = (frame > sp) & (lax.broadcasted_iota(jnp.int32, tail, 0) == 0)
    pt[3 * wide : deep] = jnp.where(hidden, -1e30, 0.0).astype(BF16)
    rest = (own, deep - 2 * wide)
    ones = jnp.where(lax.broadcasted_iota(jnp.int32, rest, 1) == wide, 1.0, 0.0).astype(BF16)
    for h in range(heads):
        left[h, :, 2 * wide : deep] = ones

    def level(r, a):
        value = gath_ref[r, (1 + a) * lat : (2 + a) * lat].astype(F32)
        if a == 0 and r > 0:
            value = value + gath_ref[r - 1, 3 * lat : 4 * lat].astype(F32)
        if a == 1 and r < count - 1:
            value = value + gath_ref[r + 1, 0:lat].astype(F32)
        return value

    loads[0].wait()
    joint = max(1, 128 // half)
    for r in range(0, count, joint):
        rows = [jnp.concatenate([level(r + j, 0), level(r + j, 1)], axis=0) for j in range(joint)]
        if joint == 1:
            even, odds = rows[0][:, :half], rows[0][:, half:]
        else:
            turn = lax.broadcasted_iota(jnp.int32, rows[0].shape, 1)
            even = jnp.where(turn < half, rows[0], pltpu.roll(rows[1], half, 1))
            odds = jnp.where(turn < half, pltpu.roll(rows[0], half, 1), rows[1])
        block = jnp.concatenate([even, odds], axis=0).astype(BF16)
        at = slice(r * half, (r + joint) * half)
        for i in range(3):
            pt[i * wide : (i + 1) * wide, at] = block
        pf[:, at] = block.astype(F32)

    patches = pt[0:wide]
    mine16 = dot_nt(pick, patches).astype(BF16)
    for copy in loads[1:]:
        copy.wait()

    span = min(tokens, 256)
    for at in range(0, tokens, span):
        cols = slice(at, at + span)
        spread = dot(gram_ref[...], pt[0 : 3 * wide, cols]).reshape(heads + 1, wide, span)
        norm[:, cols] = jnp.maximum(jnp.sum(spread * pf[:, cols][None], axis=1), 0.0)
    rs = lax.rsqrt(norm[0:1] + EPS)
    own_rs = jnp.sum(jnp.where(lane == want, rs, 0.0), axis=1, keepdims=True)

    def project(w):
        parts = [dot(mine16, m_ref[i, w]) for i in range(share)]
        return jnp.concatenate(parts, axis=1) * own_rs

    def matrix(w, h):
        return m_ref[h // per, w, :, (h % per) * hsize : (h % per + 1) * hsize]

    val_ref[...] = project(2).astype(BF16)
    raw_k = project(1)
    raw_q = project(0)
    pn[...] = (pf[...] * rs).astype(BF16)
    scale = hsize ** (-0.5) * math.log2(math.e)

    def unit(value):
        return value * lax.rsqrt(jnp.mean(value * value, axis=1, keepdims=True) + EPS)

    side = lax.broadcasted_iota(jnp.int32, (own, 2 * wide), 1)
    for h in range(heads):
        cols = slice(h * hsize, (h + 1) * hsize)
        key_ref[:, cols] = (unit(raw_k[:, cols]) * kg_ref[...]).astype(BF16)
        q = (unit(raw_q[:, cols]) * qg_ref[...] * (kg_ref[...] * scale)).astype(BF16)
        mk = matrix(1, h)
        narrow = dot_nt(q, jnp.concatenate([mk, mk], axis=0))
        top = narrow.astype(BF16).astype(F32)
        left[h, :, 0 : 2 * wide] = jnp.where(side < wide, top, narrow - top).astype(BF16)
    early = [
        pltpu.make_async_copy(key_ref, key_hbm, out_sem.at[0]),
        pltpu.make_async_copy(val_ref, val_hbm, out_sem.at[1]),
    ]
    for copy in early:
        copy.start()
    factor[...] = rs * lax.rsqrt(rs * rs * norm[1 : heads + 1] + EPS)

    def score(step):
        rows = left[step * pair : (step + 1) * pair].reshape(pair * own, deep)
        return dot(rows, pt[...])

    steps = heads // pair
    ahead = score(0)
    mixed, sums = [], []
    for step in range(steps):
        scores = ahead
        if step + 1 < steps:
            ahead = score(step + 1)
        soft, totals = [], []
        for j in range(pair):
            h = step * pair + j
            part = scores[j * own : (j + 1) * own] * factor[h : h + 1]
            peak = jnp.max(part, axis=1, keepdims=True)
            weights = jnp.exp2(part - peak)
            totals.append(jnp.sum(weights, axis=1, keepdims=True))
            soft.append(weights.astype(BF16))
        mixed.append(dot_nt(jnp.concatenate(soft, axis=0), pn[...]).astype(BF16))
        sums.append(totals)
    for h in range(heads):
        step, j = divmod(h, pair)
        out = dot(mixed[step][j * own : (j + 1) * own], matrix(2, h))
        att_ref[:, h * hsize : (h + 1) * hsize] = (out / sums[step][j]).astype(BF16)

    late = pltpu.make_async_copy(att_ref, att_hbm, out_sem.at[2])
    late.start()
    for copy in early + [late]:
        copy.wait()


def on_device(
    frames_in,
    conv_weight,
    conv_out_weight,
    embed_weight,
    norm_gain,
    q_weight,
    k_weight,
    v_weight,
    q_gain,
    k_gain,
):
    count, groups = lax.axis_size("sp"), lax.axis_size("hd")
    nframe, own_rows, ncol, cl = frames_in.shape
    if own_rows != 2 or nframe != count or count & (count - 1):
        raise ValueError("unsupported shape")
    cin, width = conv_weight.shape[-2:]
    lat = conv_out_weight.shape[-1]
    wide = 4 * lat
    depth, hw = q_weight.shape
    pos = nframe * ncol
    hsize = q_gain.shape[0]
    w2 = conv_out_weight.transpose(0, 1, 2, 4, 3)
    dma = pltpu.SemaphoreType.DMA
    heads = hw // hsize
    share = 4 if heads % 4 == 0 and count >= 4 else 1
    quarter = hw // share
    gath, m, gram = pl.pallas_call(
        functools.partial(encode_kernel, count, groups, share),
        out_shape=(
            jax.ShapeDtypeStruct((count, groups, wide // groups, pos), BF16),
            jax.ShapeDtypeStruct((share, 3, wide, quarter), BF16),
            jax.ShapeDtypeStruct(((hw // hsize + 1) * wide, 3 * wide), BF16),
        ),
        in_specs=[ANY_SPEC] * 8,
        out_specs=(ANY_SPEC,) * 3,
        scratch_shapes=[
            pltpu.VMEM((groups, 4, nframe, ncol, cl), BF16),
            pltpu.VMEM((3, 3, 3, cin, width), BF16),
            pltpu.VMEM((3, 3, 3, lat, width), BF16),
            pltpu.VMEM((wide, depth), BF16),
            pltpu.VMEM((1, depth), F32),
            pltpu.VMEM((3, depth, quarter), BF16),
            pltpu.VMEM((wide, depth), BF16),
            pltpu.VMEM((share, 3, wide, quarter), BF16),
            pltpu.VMEM(((hw // hsize + 1) * wide, 3 * wide), BF16),
            pltpu.VMEM((groups, 4, (nframe + 2) * ncol, cl), BF16),
            pltpu.VMEM((3, 2 * pos, width), F32),
            pltpu.VMEM((9 * pos, pos), BF16),
            pltpu.VMEM((groups, wide // groups, pos), F32),
            pltpu.VMEM((groups, wide // groups, pos), F32),
            pltpu.VMEM((count, groups, wide // groups, pos), BF16),
            pltpu.SemaphoreType.REGULAR((count.bit_length() - 1,)),
            dma((5,)),
            dma((3,)),
            dma((3 * SPLIT,)),
            dma((3,)),
            dma((2,)),
            dma((2,)),
            dma((groups,)),
            dma((groups,)),
            dma((groups, 2)),
            dma((groups, 2)),
            dma((groups,)),
            dma((groups,)),
            dma((count,)),
            dma((count,)),
            dma((groups,)),
            dma((groups,)),
            dma((share,)),
            dma((share,)),
        ],
        compiler_params=pltpu.CompilerParams(
            collective_id=0, has_side_effects=True, vmem_limit_bytes=60 * 1024 * 1024
        ),
    )(
        frames_in,
        conv_weight,
        w2,
        embed_weight.reshape(wide, depth),
        norm_gain.reshape(1, -1),
        q_weight,
        k_weight,
        v_weight,
    )
    own = count * (ncol // 2)
    tokens = count * pos // 2
    shape = jax.ShapeDtypeStruct((own, hw), BF16)
    return pl.pallas_call(
        functools.partial(attend_kernel, count, ncol // 2),
        out_shape=(shape,) * 3,
        in_specs=[ANY_SPEC] * 5,
        out_specs=(ANY_SPEC,) * 3,
        scratch_shapes=[
            pltpu.VMEM((count, wide, pos), BF16),
            pltpu.VMEM((share, 3, wide, quarter), BF16),
            pltpu.VMEM(((heads + 1) * wide, 3 * wide), BF16),
            pltpu.VMEM((1, hsize), F32),
            pltpu.VMEM((1, hsize), F32),
            pltpu.VMEM((own, hw), BF16),
            pltpu.VMEM((own, hw), BF16),
            pltpu.VMEM((own, hw), BF16),
            pltpu.VMEM((3 * wide + 16, tokens), BF16),
            pltpu.VMEM((wide, tokens), F32),
            pltpu.VMEM((wide, tokens), BF16),
            pltpu.VMEM((heads + 1, tokens), F32),
            pltpu.VMEM((heads, tokens), F32),
            pltpu.VMEM((heads, own, 3 * wide + 16), BF16),
            dma((5,)),
            dma((3,)),
        ],
        compiler_params=pltpu.CompilerParams(vmem_limit_bytes=67043328),
    )(
        gath.reshape(count, wide, pos),
        m,
        gram,
        q_gain.reshape(1, -1),
        k_gain.reshape(1, -1),
    )


def solution(mesh):
    in_specs = (
        P(None, "sp", None, "hd"),
        P(None, None, None, None, "hd"),
        P(None, None, None, "hd", None),
        P(),
        P(),
        P(None, "hd"),
        P(None, "hd"),
        P(None, "hd"),
        P(),
        P(),
    )
    out_specs = (P("sp", "hd"), P("sp", "hd"), P("sp", "hd"))
    return jax.shard_map(
        on_device, mesh=mesh, in_specs=in_specs, out_specs=out_specs, check_vma=False
    )
```
